512 devices in a mesh: img: 32 (over y_hi, z), sp: 16 (over y_lo, x, core).
Axes of the slice: x: 4, y: 4 (y_hi: 2, y_lo: 2; y = y_hi * 2 + y_lo), z: 16, core: 2. Of those that a mesh axis runs over, the one named last changes fastest.
Arguments:
- patches: bfloat16 [65536, 1280], P(('img', 'sp')), parts along dimension 0, may hold values from -6 to 6
- pos_ids: int32 [2, 65536], P(None, 'img'), parts along dimension 1, may hold values from 0 to 127, as said below
- norm_gain: float32 [1280], replicated, may hold values from 0.5 to 1.5
- norm_bias: float32 [1280], replicated, may hold values from -3 to 3
- qkv_weight: bfloat16 [1280, 3, 1280], P(None, None, 'sp')
- qkv_bias: float32 [3, 1280], replicated, may hold values from -3 to 3
- proj_weight: bfloat16 [1280, 1280], P('sp'), may hold values from -0.15625 to 0.15625
- proj_bias: float32 [1280], replicated, may hold values from -3 to 3
- merge_gain: float32 [1280], replicated, may hold values from 0.5 to 1.5
- merge_bias: float32 [1280], replicated, may hold values from -3 to 3
- fc1_weight: bfloat16 [5120, 5120], P(None, 'sp'), may hold values from -0.078125 to 0.078125
- fc1_bias: float32 [5120], P('sp'), may hold values from -3 to 3
Outputs:
- vit_out: bfloat16 [65536, 1280], P(('img', 'sp')), parts along dimension 0
- merged_hidden: bfloat16 [16384, 5120], P('img', 'sp'), parts along dimension 0
The draws below stay inside these ranges and needn't reach their ends.
There are 32 independent parts, one for each index of `img`. The reference program is written for one: setup_inputs(seed, part) draws one part's arguments, and reference() takes and returns one part's arrays. A program takes and returns all parts, laid end to end along the dimension named above; an argument that names none is the same for every part. Nothing has to cross between parts.
Inputs may be any that keep to these rules, and one draw needn't show every extreme that they name: pos_ids[0] and pos_ids[1] are the row and column of each patch on a grid of 2 R by 2 C patches, where the grid of 2x2 blocks has R rows and C columns, R C = 512, and one of R and C equals min(8, 512); each aligned run of 4 patches is one 2x2 block in row-major order inside it; every block of the grid appears once, in the order that the argument gives.
All inputs are finite; a program needn't handle non-finite values.
Results may differ from the reference program's by a relative error of at most 0.006.
Values may be sent and summed in bfloat16 or wider, within the bound.
A program may use at most 64 MiB of HBM per device.

```python
import jax
import jax.numpy as jnp
from jax import lax

D = 1280
HEADS = 16
MERGE_WIDTH = 5120
PATCHES = 2048
MERGED = 512


def draw_pos_ids(key, part):
    short_side = min(8, MERGED)
    long_side = MERGED // short_side
    table = jnp.array([short_side, long_side], jnp.int32)
    pick = jax.random.randint(jax.random.fold_in(key, 11), (), 0, 2)
    block_width = table[pick]
    order = jax.random.permutation(jax.random.fold_in(key, 13), MERGED).astype(jnp.int32)
    index = jnp.arange(PATCHES, dtype=jnp.int32)
    block = order[index // 4]
    inner = index % 4
    block_row = block // block_width
    block_col = block % block_width
    row = 2 * block_row + inner // 2
    col = 2 * block_col + inner % 2
    return jnp.stack([row, col]).astype(jnp.int32)


def draw_qkv_weight(key, part):
    base = jax.random.normal(key, (D, 3, D), jnp.float32) / jnp.sqrt(jnp.float32(D))
    return base.astype(jnp.bfloat16)


def block_scale(stream_key, extent, shards, smallest, top_value):
    loudness, own = 1.0, jax.random.fold_in(stream_key, 6)
    for dim, parts in shards:
        heights = jnp.exp(jax.random.uniform(jax.random.fold_in(own, dim), (parts,), jnp.float32, smallest / len(shards), top_value / len(shards)))
        loudness = loudness * jnp.repeat(heights, extent[dim] // parts).reshape([-1 if axis == dim else 1 for axis in range(len(extent))])
    return loudness


def bell_draw(stream_key, dims, spread, reach, cuts=(), held_as=jnp.bfloat16):
    values = jax.random.normal(stream_key, dims, jnp.float32) * spread
    if len(cuts) > 0:
        values = block_scale(stream_key, dims, cuts, -0.22, 0.18) * values
    return jnp.clip(values, min=-reach, max=reach).astype(held_as)


def setup_inputs(seed: int = 0, part: int = 0) -> dict:
    key_of = jax.random.split(jax.random.key(seed), 13)
    part_splits = jax.random.split(jax.random.fold_in(key_of[12], part), 13)
    patches = bell_draw(part_splits[0], (PATCHES, D), 1.0, 6.0, ((0, 16),))
    pos_ids = draw_pos_ids(jax.random.fold_in(jax.random.fold_in(key_of[12], part), 71), part)
    norm_gain = jnp.clip(1.0 + 0.1 * jax.random.normal(key_of[2], (D,), jnp.float32), 0.5, 1.5)
    norm_bias = bell_draw(key_of[3], (D,), 0.5, 3.0, (), jnp.float32)
    qkv_weight = draw_qkv_weight(jax.random.fold_in(key_of[12], 71), part)
    qkv_bias = bell_draw(key_of[5], (3, D), 0.5, 3.0, (), jnp.float32)
    proj_weight = bell_draw(key_of[6], (D, D), D ** -0.5, 0.15625, ((0, 16),))
    proj_bias = bell_draw(key_of[7], (D,), 0.5, 3.0, (), jnp.float32)
    merge_gain = jnp.clip(1.0 + 0.1 * jax.random.normal(key_of[8], (D,), jnp.float32), 0.5, 1.5)
    merge_bias = bell_draw(key_of[9], (D,), 0.5, 3.0, (), jnp.float32)
    fc1_weight = bell_draw(key_of[10], (MERGE_WIDTH, MERGE_WIDTH), MERGE_WIDTH ** -0.5, 0.078125, ((1, 16),))
    fc1_bias = bell_draw(key_of[11], (MERGE_WIDTH,), 0.5, 3.0, ((0, 16),), jnp.float32)
    return dict(patches=patches, pos_ids=pos_ids, norm_gain=norm_gain, norm_bias=norm_bias, qkv_weight=qkv_weight, qkv_bias=qkv_bias, proj_weight=proj_weight, proj_bias=proj_bias, merge_gain=merge_gain, merge_bias=merge_bias, fc1_weight=fc1_weight, fc1_bias=fc1_bias)


def layer_norm(values, gain, bias):
    mean = lax.optimization_barrier(jnp.mean(values, axis=-1, keepdims=True))
    centered = values - mean
    var = lax.optimization_barrier(jnp.mean(centered * centered, axis=-1, keepdims=True))
    return centered * lax.rsqrt(var + 1e-06) * gain + bias

def rotate(values, positions, nheads):
    count = values.shape[0]
    hdim = values.shape[1] // nheads
    quarter = hdim // 4
    inv = 1.0 / 10000.0 ** (jnp.arange(quarter, dtype=jnp.float32) * 2.0 / (hdim // 2))
    rows = positions[0].astype(jnp.float32)[:, None] * inv
    cols = positions[1].astype(jnp.float32)[:, None] * inv
    angle = jnp.concatenate([rows, cols, rows, cols], axis=1)
    cosine = jnp.cos(angle)[:, None, :]
    sine = jnp.sin(angle)[:, None, :]
    shaped = values.reshape(count, nheads, hdim)
    half = hdim // 2
    turned = jnp.concatenate([-shaped[..., half:], shaped[..., :half]], axis=-1)
    return (shaped * cosine + turned * sine).reshape(count, nheads * hdim)

def reference(patches, pos_ids, norm_gain, norm_bias, qkv_weight, qkv_bias, proj_weight, proj_bias, merge_gain, merge_bias, fc1_weight, fc1_bias):
    count = patches.shape[0]
    width = patches.shape[1]
    hdim = width // HEADS
    xfloat = patches.astype(jnp.float32)
    normed = layer_norm(xfloat, norm_gain, norm_bias).astype(jnp.bfloat16)
    qkv = jnp.dot(normed, qkv_weight.reshape(width, 3 * width), preferred_element_type=jnp.float32).reshape(count, 3, width)
    qkv = qkv + qkv_bias[None]
    query = rotate(qkv[:, 0], pos_ids, HEADS).astype(jnp.bfloat16)
    keys = rotate(qkv[:, 1], pos_ids, HEADS).astype(jnp.bfloat16)
    value = qkv[:, 2].astype(jnp.bfloat16)
    qh = query.reshape(count, HEADS, hdim).transpose(1, 0, 2)
    kh = keys.reshape(count, HEADS, hdim).transpose(1, 0, 2)
    vh = value.reshape(count, HEADS, hdim).transpose(1, 0, 2)
    scale = 1.0 / jnp.sqrt(jnp.float32(hdim))

    def one_head(triple):
        qone, kone, vone = triple
        scores = jnp.dot(qone, kone.T, preferred_element_type=jnp.float32) * scale
        top = lax.optimization_barrier(jnp.max(scores, axis=-1, keepdims=True))
        expo = jnp.exp(scores - top)
        weights = (expo / lax.optimization_barrier(jnp.sum(expo, axis=-1, keepdims=True))).astype(jnp.bfloat16)
        return jnp.dot(weights, vone, preferred_element_type=jnp.float32).astype(jnp.bfloat16)
    heads_out = lax.map(one_head, (qh, kh, vh))
    attended = heads_out.transpose(1, 0, 2).reshape(count, width)
    projected = jnp.dot(attended, proj_weight, preferred_element_type=jnp.float32)
    vit_out = (xfloat + projected + proj_bias).astype(jnp.bfloat16)
    zn = layer_norm(vit_out.astype(jnp.float32), merge_gain, merge_bias).astype(jnp.bfloat16)
    blocks = zn.reshape(count // 4, 4 * width)
    hidden = jnp.dot(blocks, fc1_weight, preferred_element_type=jnp.float32) + fc1_bias
    merged_hidden = jax.nn.gelu(hidden, approximate=False).astype(jnp.bfloat16)
    return (vit_out, merged_hidden)
```

```python
import math

import jax
import jax.numpy as jnp
from jax import lax
from jax.experimental import pallas as pl
from jax.experimental.pallas import tpu as pltpu
from jax.sharding import PartitionSpec as P

MESH = pl.DeviceIdType.MESH
HEADS = 16
D = 1280
HDIM = 80
PATCHES = 2048
HIDDEN = 5120
SHARE = 320
ROLES = 8
W_CUT = ((0, 48), (48, 32))
SCALE = math.log2(math.e) / math.sqrt(HDIM)


def norm_rows(v, gain, bias):
    mean = jnp.mean(v, axis=-1, keepdims=True)
    cen = v - mean
    var = jnp.mean(cen * cen, axis=-1, keepdims=True)
    return cen * lax.rsqrt(var + 1e-06) * gain + bias


def kernel(
    x_ref, pos_ref, g1_ref, b1_ref, wq_hbm, bq_ref, wp_hbm, pb_ref, g2_ref, b2_ref, fc_hbm, fb_ref,
    vit_hbm, hid_hbm,
    gat, blk, wg, att, osend, qt, kk, vt, sc, fcv, wqv, bcol, fcol, zf, vitv, hidv,
    send, recv, asend, arecv, local,
):
    me = lax.axis_index("sp")
    core = me % 2
    mx = (me // 2) % 4
    my = me // 8

    def dev(dx, dy, p):
        return ((my + dy) % 2) * 8 + ((mx + dx) % 4) * 2 + (core + p) % 2

    wq_copy = pltpu.make_async_copy(wq_hbm, wqv, local.at[0])
    wp_copy = pltpu.make_async_copy(wp_hbm, wg.at[0, 0], local.at[1])
    fc_copy = pltpu.make_async_copy(fc_hbm, fcv, local.at[2])
    wq_copy.start()
    wp_copy.start()
    fc_copy.start()

    xf = x_ref[...].astype(jnp.float32)
    normed = norm_rows(xf, g1_ref[...].reshape(1, D), b1_ref[...].reshape(1, D)).astype(jnp.bfloat16)
    gat[0, 0] = normed.reshape(2, 64, D)

    barrier = pltpu.get_barrier_semaphore()
    for step in range(1, 16):
        pl.semaphore_signal(barrier, inc=1, device_id={"sp": (me + step) % 16}, device_id_type=MESH)
    pl.semaphore_wait(barrier, 15)

    class Gather:
        def __init__(self, index, piece):
            self.index, self.piece, self.sends = index, piece, []

        def put(self, src, dst, dx, dy, p):
            copy = pltpu.make_async_remote_copy(
                src_ref=self.piece(*src),
                dst_ref=self.piece(*dst),
                send_sem=send.at[self.index, len(self.sends)],
                recv_sem=recv.at[self.index, *dst],
                device_id={"sp": dev(dx, dy, p)},
                device_id_type=MESH,
            )
            copy.start()
            self.sends.append(copy)

        def pass_on(self, r, h, dx, dy):
            role = 4 * ((r // 4 + dy) % 2) + (r % 4 - dx) % 4
            self.put((r, 0, h), (role, 0, h), dx, dy, 0)

        def share(self, r, h):
            self.put((r, 0, h), (r, 1, h), 0, 0, 1)

        def wait(self, r, p, h):
            pltpu.make_async_remote_copy(
                src_ref=self.piece(r, p, h),
                dst_ref=self.piece(r, p, h),
                send_sem=send.at[self.index, 0],
                recv_sem=recv.at[self.index, r, p, h],
                device_id={"sp": dev(0, 0, 1)},
                device_id_type=MESH,
            ).wait_recv()

        def wait_partner(self, roles):
            for r in roles:
                for h in range(2):
                    self.wait(r, 1, h)

        def begin(self):
            for h in range(2):
                self.pass_on(0, h, 1, 0)
                self.pass_on(0, 1 - h, -1, 0)
                self.pass_on(0, h, 0, 1)
            for h in range(2):
                self.share(0, h)

        def first(self):
            self.wait(3, 0, 0)
            self.pass_on(3, 0, 1, 0)
            self.wait(1, 0, 1)
            self.pass_on(1, 1, -1, 0)
            self.wait(4, 0, 0)
            self.pass_on(4, 0, 1, 0)
            self.pass_on(4, 0, -1, 0)
            self.share(3, 0)
            self.share(1, 1)
            self.share(4, 0)
            self.wait(4, 0, 1)
            self.pass_on(4, 1, 1, 0)
            self.pass_on(4, 1, -1, 0)
            self.wait(3, 0, 1)
            self.wait(1, 0, 0)
            self.share(4, 1)
            self.share(3, 1)
            self.share(1, 0)

        def second(self):
            for h in range(2):
                self.wait(2, 0, h)
                self.pass_on(2, h, 0, 1)
                self.share(2, h)

        def third(self, h):
            for r in (5, 7, 6):
                self.wait(r, 0, h)
                self.share(r, h)

        def drain(self):
            for copy in self.sends:
                copy.wait_send()

    g1 = Gather(0, lambda r, p, h: gat.at[r, p, h])
    gw = Gather(1, lambda r, p, h: wg.at[r, p, pl.ds(*W_CUT[h])])
    g2 = Gather(2, lambda r, p, h: blk.at[r, p, h])

    g1.begin()

    lane = lax.broadcasted_iota(jnp.int32, (HDIM, D), 1)
    sub = lax.broadcasted_iota(jnp.int32, (HDIM, D), 0)
    mine = lane == sub + me * HDIM
    for c in range(3):
        col = jnp.sum(jnp.where(mine, bq_ref[c : c + 1, :], 0.0), axis=1, keepdims=True)
        bcol[c] = jnp.broadcast_to(col, (HDIM, 128))
    same = lax.broadcasted_iota(jnp.int32, (SHARE, SHARE), 0) == lax.broadcasted_iota(
        jnp.int32, (SHARE, SHARE), 1
    )
    col = jnp.sum(jnp.where(same, fb_ref[...].reshape(1, SHARE), 0.0), axis=1, keepdims=True)
    fcol[...] = jnp.broadcast_to(col, (SHARE, 128))

    wq_copy.wait()

    def qkv(r):
        rows = gat[r].reshape(256, D)
        out = lax.dot_general(
            wqv[...], rows, (((1,), (1,)), ((), ())), preferred_element_type=jnp.float32
        )
        at = [pl.multiple_of(dev(r % 4, r // 4, p) * 128, 128) for p in range(2)]
        prow = jnp.concatenate([pos_ref[0:1, pl.ds(a, 128)] for a in at], axis=1).astype(jnp.float32)
        pcol = jnp.concatenate([pos_ref[1:2, pl.ds(a, 128)] for a in at], axis=1).astype(jnp.float32)
        row = lax.broadcasted_iota(jnp.int32, (40, 256), 0)
        power = jnp.where(row < 20, row, row - 20).astype(jnp.float32)
        inv = jnp.exp2(power * (-math.log2(10000.0) / 20.0))
        angle = jnp.where(row < 20, prow, pcol) * inv
        cos, sin = jnp.cos(angle), jnp.sin(angle)

        def turn(v):
            lo, hi = v[:40], v[40:]
            return jnp.concatenate([lo * cos - hi * sin, hi * cos + lo * sin], axis=0)

        bias = [jnp.concatenate([bcol[c], bcol[c]], axis=1) for c in range(3)]
        pad = jnp.zeros((128 - HDIM, 256), jnp.float32)
        q = turn(out[0:80] + bias[0])
        k = turn(out[80:160] + bias[1])
        v = out[160:240] + bias[2]
        qt[r] = jnp.concatenate([q, pad], axis=0).astype(jnp.bfloat16)
        kk[r] = jnp.concatenate([k, pad], axis=0).T.astype(jnp.bfloat16)
        vt[r] = v.astype(jnp.bfloat16)

    g1.wait_partner([0])
    qkv(0)
    g1.first()
    g1.wait_partner([3, 1, 4])
    for r in (3, 1, 4):
        qkv(r)
    g1.second()
    g1.wait_partner([2])
    qkv(2)
    g1.third(0)
    g1.third(1)
    wp_copy.wait()
    gw.begin()
    g1.wait_partner([5, 7, 6])
    for r in (5, 7, 6):
        qkv(r)

    def score(r, slot):
        top = None
        for kc in range(ROLES):
            s = jnp.dot(kk[kc], qt[r], preferred_element_type=jnp.float32)
            sc[slot, kc] = s
            m = jnp.max(s.reshape(32, 8, 256), axis=0)
            top = m if top is None else jnp.maximum(top, m)
        return jnp.max(top, axis=0, keepdims=True) * SCALE

    def weigh(r, slot, top):
        total, out = None, None
        for kc in range(ROLES):
            w = jnp.exp2(sc[slot, kc] * SCALE - top)
            s = jnp.sum(w.reshape(32, 8, 256), axis=0)
            o = jnp.dot(vt[kc], w.astype(jnp.bfloat16), preferred_element_type=jnp.float32)
            total = s if total is None else total + s
            out = o if out is None else out + o
        out = (out / jnp.sum(total, axis=0, keepdims=True)).astype(jnp.bfloat16)
        for p in range(2):
            osend[r, p] = out[:, p * 128 : (p + 1) * 128]

    back = []

    def give(r):
        for p in range(2):
            if r == 0 and p == 0:
                continue
            role = 4 * (r // 4) + (-r % 4) % 4
            copy = pltpu.make_async_remote_copy(
                src_ref=osend.at[r, p],
                dst_ref=att.at[role, p],
                send_sem=asend.at[r, p],
                recv_sem=arecv.at[role, p],
                device_id={"sp": dev(r % 4, r // 4, p)},
                device_id_type=MESH,
            )
            copy.start()
            back.append((copy, role, p))

    order = (6, 7, 5, 2, 4, 3, 1, 0)
    top = score(order[0], 0)
    for i, r in enumerate(order):
        if i + 1 < ROLES:
            later = score(order[i + 1], (i + 1) % 2)
        weigh(r, i % 2, top)
        top = later
        if i > 0:
            give(order[i - 1])
        if i == 3:
            gw.first()
        if i == 6:
            gw.second()
    give(order[-1])
    att[0, 0] = osend[0, 0]
    gw.third(0)
    gw.third(1)
    gw.wait_partner(range(ROLES))
    for copy, role, p in back:
        copy.wait_recv()

    got = att[...].reshape(D, 128).T
    out = jnp.dot(got, wg[...].reshape(D, D), preferred_element_type=jnp.float32)
    vit = (x_ref[...].astype(jnp.float32) + out + pb_ref[...].reshape(1, D)).astype(jnp.bfloat16)
    vitv[...] = vit
    zn = norm_rows(vit.astype(jnp.float32), g2_ref[...].reshape(1, D), b2_ref[...].reshape(1, D))
    for b in range(D // 128):
        zf[b] = zn[:, b * 128 : (b + 1) * 128]
    for j in range(4):
        for b in range(D // 128):
            blk[0, 0, j // 2, pl.ds((j % 2) * 32, 32), pl.ds(b * 128, 128)] = zf[
                b, pl.ds(j, 32, stride=4), :
            ].astype(jnp.bfloat16)

    g2.begin()
    vit_copy = pltpu.make_async_copy(vitv, vit_hbm, local.at[3])
    vit_copy.start()
    fc_copy.wait()

    def fc1(dy, h):
        total = None
        for j in (2 * h, 2 * h + 1):
            parts = []
            for ax in range(4):
                r = 4 * dy + (ax + 4 - mx) % 4
                for c in range(2):
                    parts.append(blk[r, (c + core) % 2, h, pl.ds((j % 2) * 32, 32)])
            o = lax.dot_general(
                fcv[:, j * D : (j + 1) * D],
                jnp.concatenate(parts, axis=0),
                (((1,), (1,)), ((), ())),
                preferred_element_type=jnp.float32,
            )
            total = o if total is None else total + o
        return total

    def finish(dy, total):
        v = total + jnp.concatenate([fcol[...], fcol[...]], axis=1)
        hidv[dy] = (0.5 * v * (1.0 + lax.erf(v * (2.0**-0.5)))).astype(jnp.bfloat16)
        at = pl.multiple_of(((my + dy) % 2) * 256, 256)
        copy = pltpu.make_async_copy(hidv.at[dy], hid_hbm.at[:, pl.ds(at, 256)], local.at[4 + dy])
        copy.start()
        return copy

    g2.first()
    g2.second()
    g2.wait_partner([0, 3, 1, 2])
    done0 = finish(0, fc1(0, 0) + fc1(0, 1))
    g2.third(0)
    for r in (4, 5, 7, 6):
        g2.wait(r, 1, 0)
    half = fc1(1, 0)
    g2.third(1)
    for r in (4, 5, 7, 6):
        g2.wait(r, 1, 1)
    done1 = finish(1, half + fc1(1, 1))

    for g in (g1, gw, g2):
        g.drain()
    for copy, _, _ in back:
        copy.wait_send()
    vit_copy.wait()
    done0.wait()
    done1.wait()


def per_device(
    patches, pos_ids, norm_gain, norm_bias, qkv_weight, qkv_bias, proj_weight, proj_bias, merge_gain, merge_bias,
    fc1_weight, fc1_bias,
):
    vmem = pl.BlockSpec(memory_space=pltpu.VMEM)
    hbm = pl.BlockSpec(memory_space=pl.ANY)
    bf, f32 = jnp.bfloat16, jnp.float32
    dma = pltpu.SemaphoreType.DMA
    vit, hid = pl.pallas_call(
        kernel,
        out_shape=(jax.ShapeDtypeStruct((128, D), bf), jax.ShapeDtypeStruct((SHARE, 512), bf)),
        in_specs=[vmem, vmem, vmem, vmem, hbm, vmem, hbm, vmem, vmem, vmem, hbm, vmem],
        out_specs=(hbm, hbm),
        scratch_shapes=[
            pltpu.VMEM((ROLES, 2, 2, 64, D), bf),
            pltpu.VMEM((ROLES, 2, 2, 64, D), bf),
            pltpu.VMEM((ROLES, 2, HDIM, D), bf),
            pltpu.VMEM((ROLES, 2, HDIM, 128), bf),
            pltpu.VMEM((ROLES, 2, HDIM, 128), bf),
            pltpu.VMEM((ROLES, 128, 256), bf),
            pltpu.VMEM((ROLES, 256, 128), bf),
            pltpu.VMEM((ROLES, HDIM, 256), bf),
            pltpu.VMEM((2, ROLES, 256, 256), f32),
            pltpu.VMEM((SHARE, HIDDEN), bf),
            pltpu.VMEM((3 * HDIM, D), bf),
            pltpu.VMEM((3, HDIM, 128), f32),
            pltpu.VMEM((SHARE, 128), f32),
            pltpu.VMEM((D // 128, 128, 128), f32),
            pltpu.VMEM((128, D), bf),
            pltpu.VMEM((2, SHARE, 256), bf),
            dma((3, 32)),
            dma((3, ROLES, 2, 2)),
            dma((ROLES, 2)),
            dma((ROLES, 2)),
            dma((6,)),
        ],
        compiler_params=pltpu.CompilerParams(
            collective_id=0, has_side_effects=True, vmem_limit_bytes=58 * 1024 * 1024
        ),
    )(
        patches,
        pos_ids,
        norm_gain,
        norm_bias,
        qkv_weight.transpose(1, 2, 0).reshape(3 * HDIM, D),
        qkv_bias,
        proj_weight,
        proj_bias,
        merge_gain,
        merge_bias,
        fc1_weight.T,
        fc1_bias,
    )
    return vit, hid.T


def solution(mesh):
    return jax.shard_map(
        per_device,
        mesh=mesh,
        in_specs=(
            P(("img", "sp"), None),
            P(None, "img"),
            P(),
            P(),
            P(None, None, "sp"),
            P(),
            P("sp", None),
            P(),
            P(),
            P(),
            P(None, "sp"),
            P("sp"),
        ),
        out_specs=(P(("img", "sp"), None), P("img", "sp")),
        check_vma=False,
    )
```

```python
import math

import jax
import jax.numpy as jnp
from jax import lax
from jax.experimental import pallas as pl
from jax.experimental.pallas import tpu as pltpu
from jax.sharding import PartitionSpec as P

MESH = pl.DeviceIdType.MESH
HEADS = 16
D = 1280
HDIM = 80
PATCHES = 2048
HIDDEN = 5120
SHARE = 320
ROLES = 8
SCALE = math.log2(math.e) / math.sqrt(HDIM)


def norm_rows(v, gain, bias):
    mean = jnp.mean(v, axis=-1, keepdims=True)
    cen = v - mean
    var = jnp.mean(cen * cen, axis=-1, keepdims=True)
    return cen * lax.rsqrt(var + 1e-06) * gain + bias


def kernel(
    x_ref, pos_ref, g1_ref, b1_ref, wq_hbm, bq_ref, wp_hbm, pb_ref, g2_ref, b2_ref, fc_hbm, fb_ref,
    vit_ref, hid_ref,
    gat, blk, wg, att, osend, qt, kk, vt, sc, fcv, wqv, bcol, fcol, zf,
    ssend, srecv, precv, wsrecv, wprecv, asem, local,
):
    me = lax.axis_index("sp")
    core = me % 2
    mx = (me // 2) % 4
    my = me // 8

    def dev(dx, dy, p):
        return ((my + dy) % 2) * 8 + ((mx + dx) % 4) * 2 + (core + p) % 2

    barrier = pltpu.get_barrier_semaphore()
    for step in range(1, 16):
        pl.semaphore_signal(barrier, inc=1, device_id={"sp": (me + step) % 16}, device_id_type=MESH)

    wq_copy = pltpu.make_async_copy(wq_hbm, wqv, local.at[0])
    wp_copy = pltpu.make_async_copy(wp_hbm, wg.at[0, 0], local.at[1])
    fc_copy = pltpu.make_async_copy(fc_hbm, fcv, local.at[2])
    wq_copy.start()
    wp_copy.start()
    fc_copy.start()

    xf = x_ref[...].astype(jnp.float32)
    normed = norm_rows(xf, g1_ref[...].reshape(1, D), b1_ref[...].reshape(1, D)).astype(jnp.bfloat16)
    gat[0, 0] = normed

    pl.semaphore_wait(barrier, 15)

    class Gather:
        def __init__(self, ref, up, down, across, flow, groups, parts, srecv, precv, ssend):
            self.ref, self.up, self.down, self.across, self.flow = ref, up, down, across, flow
            self.groups, self.parts, self.srecv, self.precv, self.ssend = groups, parts, srecv, precv, ssend
            self.rows, self.here, self.sem = 0, {}, {}
            for r in range(1, ROLES):
                for g in groups[r]:
                    for i in g:
                        self.sem[r, i] = len(set(self.sem.values())) if i == g[0] else self.sem[r, g[0]]

        def copy(self, src, dst, size, at, rsem, dx, dy, p):
            return pltpu.make_async_remote_copy(
                src_ref=self.ref.at[src[0], src[1], pl.ds(at, size)],
                dst_ref=self.ref.at[dst[0], dst[1], pl.ds(at, size)],
                send_sem=self.ssend,
                recv_sem=rsem,
                device_id={"sp": dev(dx, dy, p)},
                device_id_type=MESH,
            )

        def pass_on(self, r, i, dx, dy):
            role = 4 * ((r // 4 + dy) % 2) + (r % 4 - dx) % 4
            self.copy((r, 0), (role, 0), 16, 16 * i, self.srecv.at[self.sem[role, i]], dx, dy, 0).start()
            self.rows += 16

        def share(self, r, part):
            at, size, which = self.parts[part]
            self.copy((r, 0), (r, 1), size, at, self.precv.at[r, which], 0, 0, 1).start()
            self.rows += size

        def wait(self, r, g):
            self.copy((r, 0), (r, 0), 16 * len(g), 16 * g[0], self.srecv.at[self.sem[r, g[0]]], 0, 0, 1).wait_recv()
            assert list(g) in [list(v) for v in self.groups[r]]
            if r in (1, 3) and self.across in g:
                self.pass_on(r, self.across, 0, 1)
            here = self.here.setdefault(r, set())
            for part, (at, size, _) in enumerate(self.parts):
                mine = set(range(at // 16, (at + size) // 16))
                if mine <= here | set(g) and not mine <= here:
                    self.share(r, part)
            here.update(g)

        def wait_partner(self, r, which=0):
            size = sum(v[1] for v in self.parts if v[2] == which)
            at = min(v[0] for v in self.parts if v[2] == which)
            self.copy((r, 1), (r, 1), size, at, self.precv.at[r, which], 0, 0, 1).wait_recv()

        def begin(self):
            for a, b, c in zip(self.up + self.down, self.down + self.up, self.flow):
                self.pass_on(0, a, 1, 0)
                self.pass_on(0, b, -1, 0)
                self.pass_on(0, c, 0, 1)
            for part in range(len(self.parts)):
                self.share(0, part)

        def ring(self, r, i):
            self.wait(r, [i])
            self.pass_on(r, i, 1 if r == 3 else -1, 0)

        def cross(self, g):
            self.wait(4, g)
            for i in g:
                if i != self.across:
                    self.pass_on(4, i, 1, 0)
                    self.pass_on(4, i, -1, 0)

        def rest(self):
            for r, done in ((3, self.up), (1, self.down)):
                for g in self.groups[r]:
                    if g[0] not in done:
                        self.wait(r, g)

        def far(self, i):
            self.wait(2, [i])
            self.pass_on(2, i, 0, 1)

        def last(self, g):
            for r in (5, 7, 6):
                self.wait(r, g)

        def drain(self):
            size = self.ref.shape[2]
            assert self.rows == 15 * size
            flat = self.ref.reshape(16 * size, D).at[pl.ds(0, self.rows)]
            pltpu.make_async_remote_copy(
                src_ref=flat, dst_ref=flat, send_sem=self.ssend, recv_sem=self.precv.at[0, 0],
                device_id={"sp": dev(0, 0, 1)}, device_id_type=MESH,
            ).wait_send()

    halves = [[0, 1, 2, 3], [4, 5, 6, 7]]
    groups = {
        1: [[2], [3], [6], [7], [0, 1], [4, 5]],
        2: [[i] for i in range(8)],
        3: [[0], [1], [4], [5], [2, 3], [6], [7]],
        4: halves, 5: halves, 6: halves, 7: halves,
    }
    flow = [0, 2, 1, 3, 4, 6, 5, 7]
    big = ([0, 1, 4, 5], [2, 3, 6, 7], 7, flow, groups)
    g1 = Gather(gat, *big, [(32 * j, 32, 0) for j in range(4)], srecv, precv, ssend.at[0])
    g2 = Gather(blk, *big, [(32 * j, 32, j // 2) for j in range(4)], srecv, precv, ssend.at[1])
    whole = [[0, 1, 2, 3, 4]]
    wgroups = {
        1: [[4], [3], [0, 1, 2]],
        2: [[i] for i in range(5)],
        3: [[i] for i in range(5)],
        4: [[0, 1, 2], [3, 4]], 5: whole, 6: whole, 7: whole,
    }
    gw = Gather(wg, [0, 1, 2], [4, 3], 4, [0, 1, 2, 3, 4], wgroups, [(0, 80, 0)], wsrecv, wprecv, ssend.at[2])

    g1.begin()

    lane = lax.broadcasted_iota(jnp.int32, (HDIM, D), 1)
    sub = lax.broadcasted_iota(jnp.int32, (HDIM, D), 0)
    mine = lane == sub + me * HDIM
    for c in range(3):
        col = jnp.sum(jnp.where(mine, bq_ref[c : c + 1, :], 0.0), axis=1, keepdims=True)
        bcol[c] = jnp.broadcast_to(col, (HDIM, 128))
    same = lax.broadcasted_iota(jnp.int32, (SHARE, SHARE), 0) == lax.broadcasted_iota(
        jnp.int32, (SHARE, SHARE), 1
    )
    col = jnp.sum(jnp.where(same, fb_ref[...].reshape(1, SHARE), 0.0), axis=1, keepdims=True)
    fcol[...] = jnp.broadcast_to(col, (SHARE, 128))

    wq_copy.wait()

    def qkv(r):
        rows = gat[r].reshape(256, D)
        out = lax.dot_general(
            wqv[...], rows, (((1,), (1,)), ((), ())), preferred_element_type=jnp.float32
        )
        at = [pl.multiple_of(dev(r % 4, r // 4, p) * 128, 128) for p in range(2)]
        prow = jnp.concatenate([pos_ref[0:1, pl.ds(a, 128)] for a in at], axis=1).astype(jnp.float32)
        pcol = jnp.concatenate([pos_ref[1:2, pl.ds(a, 128)] for a in at], axis=1).astype(jnp.float32)
        row = lax.broadcasted_iota(jnp.int32, (40, 256), 0)
        power = jnp.where(row < 20, row, row - 20).astype(jnp.float32)
        inv = jnp.exp2(power * (-math.log2(10000.0) / 20.0))
        angle = jnp.where(row < 20, prow, pcol) * inv
        cos, sin = jnp.cos(angle), jnp.sin(angle)

        def turn(v):
            lo, hi = v[:40], v[40:]
            return jnp.concatenate([lo * cos - hi * sin, hi * cos + lo * sin], axis=0)

        bias = [jnp.concatenate([bcol[c], bcol[c]], axis=1) for c in range(3)]
        pad = jnp.zeros((128 - HDIM, 256), jnp.float32)
        q = turn(out[0:80] + bias[0])
        k = turn(out[80:160] + bias[1])
        v = out[160:240] + bias[2]
        qt[r] = jnp.concatenate([q, pad], axis=0).astype(jnp.bfloat16)
        kk[r] = jnp.concatenate([k, pad], axis=0).T.astype(jnp.bfloat16)
        vt[r] = v.astype(jnp.bfloat16)

    with jax.named_scope("a_own"):
        g1.wait_partner(0)
        qkv(0)
    with jax.named_scope("a_ring"):
        for i, j in zip(g1.up, g1.down):
            g1.ring(3, i)
            g1.ring(1, j)
    with jax.named_scope("a_cross"):
        g1.cross(halves[0])
    with jax.named_scope("a_rest"):
        g1.rest()
        g1.cross(halves[1])
    with jax.named_scope("a_far"):
        for i in flow:
            g1.far(i)
    with jax.named_scope("a_wbegin"):
        wp_copy.wait()
        gw.begin()
    with jax.named_scope("a_qkv"):
        for r in (3, 1, 4, 2):
            g1.wait_partner(r)
            qkv(r)
    with jax.named_scope("a_last0"):
        g1.last(halves[0])
    with jax.named_scope("a_last1"):
        g1.last(halves[1])
    with jax.named_scope("w_ring0"):
        gw.ring(3, 0)
        gw.ring(1, 4)
    with jax.named_scope("a_qkv2"):
        g1.wait_partner(5)
        qkv(5)
        g1.wait_partner(7)
        qkv(7)
    with jax.named_scope("w_ring1"):
        gw.ring(3, 1)
        gw.ring(1, 3)
    with jax.named_scope("a_qkv3"):
        g1.wait_partner(6)
        qkv(6)

    def score(r, slot):
        top = None
        for kc in range(ROLES):
            s = jnp.dot(kk[kc], qt[r], preferred_element_type=jnp.float32)
            sc[slot, kc] = s
            m = jnp.max(s.reshape(32, 8, 256), axis=0)
            top = m if top is None else jnp.maximum(top, m)
        return jnp.max(top, axis=0, keepdims=True) * SCALE

    def weigh(r, slot, top):
        total, out = None, None
        for kc in range(ROLES):
            w = jnp.exp2(sc[slot, kc] * SCALE - top)
            s = jnp.sum(w.reshape(32, 8, 256), axis=0)
            o = jnp.dot(vt[kc], w.astype(jnp.bfloat16), preferred_element_type=jnp.float32)
            total = s if total is None else total + s
            out = o if out is None else out + o
        out = (out / jnp.sum(total, axis=0, keepdims=True)).astype(jnp.bfloat16)
        for p in range(2):
            osend[2 * r + p] = out[:, p * 128 : (p + 1) * 128]

    def give(r):
        for p in range(2):
            if r == 0 and p == 0:
                continue
            role = 4 * (r // 4) + (-r % 4) % 4
            pltpu.make_async_remote_copy(
                src_ref=osend.at[2 * r + p],
                dst_ref=att.at[2 * role + p],
                send_sem=asem.at[0],
                recv_sem=asem.at[1],
                device_id={"sp": dev(r % 4, r // 4, p)},
                device_id_type=MESH,
            ).start()

    order = (6, 7, 5, 2, 4, 3, 1, 0)
    top = score(order[0], 0)
    for i, r in enumerate(order):
        if i + 1 < ROLES:
            later = score(order[i + 1], (i + 1) % 2)
        weigh(r, i % 2, top)
        top = later
        if i > 0:
            give(order[i - 1])
        with jax.named_scope(f"w_tile{i}"):
            if i == 0:
                gw.ring(3, 2)
            if i == 1:
                gw.cross([0, 1, 2])
            if i == 2:
                gw.cross([3, 4])
                gw.rest()
            if i == 3:
                gw.far(0)
                gw.far(4)
            if i == 4:
                gw.far(1)
                gw.far(3)
            if i == 5:
                gw.far(2)
    with jax.named_scope("t_give"):
        give(order[-1])
        att[0] = osend[0]
    with jax.named_scope("w_last"):
        gw.last(whole[0])
    with jax.named_scope("w_partner"):
        for r in range(ROLES):
            gw.wait_partner(r)
    with jax.named_scope("t_back"):
        pltpu.make_async_remote_copy(
            src_ref=osend.at[pl.ds(1, 15)], dst_ref=att.at[pl.ds(1, 15)], send_sem=asem.at[0], recv_sem=asem.at[1],
            device_id={"sp": dev(0, 0, 1)}, device_id_type=MESH,
        ).wait_recv()

    got = att[...].reshape(D, 128).T
    out = jnp.dot(got, wg[...].reshape(D, D), preferred_element_type=jnp.float32)
    vit = (x_ref[...].astype(jnp.float32) + out + pb_ref[...].reshape(1, D)).astype(jnp.bfloat16)
    vit_ref[...] = vit
    zn = norm_rows(vit.astype(jnp.float32), g2_ref[...].reshape(1, D), b2_ref[...].reshape(1, D))
    for b in range(D // 128):
        zf[b] = zn[:, b * 128 : (b + 1) * 128]
    for j in range(4):
        for b in range(D // 128):
            blk[0, 0, pl.ds(j * 32, 32), pl.ds(b * 128, 128)] = zf[
                b, pl.ds(j, 32, stride=4), :
            ].astype(jnp.bfloat16)

    g2.begin()
    fc_copy.wait()

    def fc1(dy, j):
        parts = []
        for ax in range(4):
            r = 4 * dy + (ax + 4 - mx) % 4
            for c in range(2):
                parts.append(blk[r, (c + core) % 2, pl.ds(j * 32, 32)])
        return lax.dot_general(
            fcv[:, j * D : (j + 1) * D],
            jnp.concatenate(parts, axis=0),
            (((1,), (1,)), ((), ())),
            preferred_element_type=jnp.float32,
        )

    def finish(dy, total):
        v = total + jnp.concatenate([fcol[...], fcol[...]], axis=1)
        at = pl.multiple_of(((my + dy) % 2) * 256, 256)
        hid_ref[:, pl.ds(at, 256)] = (0.5 * v * (1.0 + lax.erf(v * (2.0**-0.5)))).astype(jnp.bfloat16)

    with jax.named_scope("b_ring"):
        for i, j in zip(g2.up, g2.down):
            g2.ring(3, i)
            g2.ring(1, j)
    with jax.named_scope("b_cross"):
        g2.cross(halves[0])
    with jax.named_scope("b_rest"):
        g2.rest()
        g2.cross(halves[1])
    with jax.named_scope("b_far"):
        for i in flow:
            g2.far(i)
    with jax.named_scope("b_far_p"):
        for r in (0, 3, 1, 2):
            g2.wait_partner(r, 0)
            g2.wait_partner(r, 1)
    with jax.named_scope("b_fc1"):
        finish(0, fc1(0, 0) + fc1(0, 1) + fc1(0, 2) + fc1(0, 3))
    with jax.named_scope("b_last0"):
        g2.last(halves[0])
    with jax.named_scope("b_last0_p"):
        for r in (4, 5, 7, 6):
            g2.wait_partner(r, 0)
    with jax.named_scope("b_fc1_0"):
        half = fc1(1, 0) + fc1(1, 1)
    with jax.named_scope("b_last1"):
        g2.last(halves[1])
    with jax.named_scope("b_last1_p"):
        for r in (4, 5, 7, 6):
            g2.wait_partner(r, 1)
    with jax.named_scope("b_fc1_1"):
        finish(1, half + fc1(1, 2) + fc1(1, 3))

    with jax.named_scope("drain"):
        for g in (g1, gw, g2):
            g.drain()
        pltpu.make_async_remote_copy(
            src_ref=osend.at[pl.ds(1, 15)], dst_ref=att.at[pl.ds(1, 15)], send_sem=asem.at[0], recv_sem=asem.at[1],
            device_id={"sp": dev(0, 0, 1)}, device_id_type=MESH,
        ).wait_send()


def per_device(
    patches, pos_ids, norm_gain, norm_bias, qkv_weight, qkv_bias, proj_weight, proj_bias, merge_gain, merge_bias,
    fc1_weight, fc1_bias,
):
    vmem = pl.BlockSpec(memory_space=pltpu.VMEM)
    hbm = pl.BlockSpec(memory_space=pl.ANY)
    bf, f32 = jnp.bfloat16, jnp.float32
    dma = pltpu.SemaphoreType.DMA
    vit, hid = pl.pallas_call(
        kernel,
        out_shape=(pltpu.VMEM((128, D), bf), pltpu.VMEM((SHARE, 512), bf)),
        in_specs=[vmem, vmem, vmem, vmem, hbm, vmem, hbm, vmem, vmem, vmem, hbm, vmem],
        out_specs=(vmem, vmem),
        scratch_shapes=[
            pltpu.VMEM((ROLES, 2, 128, D), bf),
            pltpu.VMEM((ROLES, 2, 128, D), bf),
            pltpu.VMEM((ROLES, 2, HDIM, D), bf),
            pltpu.VMEM((2 * ROLES, HDIM, 128), bf),
            pltpu.VMEM((2 * ROLES, HDIM, 128), bf),
            pltpu.VMEM((ROLES, 128, 256), bf),
            pltpu.VMEM((ROLES, 256, 128), bf),
            pltpu.VMEM((ROLES, HDIM, 256), bf),
            pltpu.VMEM((2, ROLES, 256, 256), f32),
            pltpu.VMEM((SHARE, HIDDEN), bf),
            pltpu.VMEM((3 * HDIM, D), bf),
            pltpu.VMEM((3, HDIM, 128), f32),
            pltpu.VMEM((SHARE, 128), f32),
            pltpu.VMEM((D // 128, 128, 128), f32),
            dma((3,)),
            dma((29,)),
            dma((ROLES, 2)),
            dma((18,)),
            dma((ROLES, 1)),
            dma((2,)),
            dma((3,)),
        ],
        compiler_params=pltpu.CompilerParams(
            collective_id=0, has_side_effects=True, vmem_limit_bytes=58 * 1024 * 1024
        ),
    )(
        patches,
        pos_ids,
        norm_gain,
        norm_bias,
        qkv_weight.transpose(1, 2, 0).reshape(3 * HDIM, D),
        qkv_bias,
        proj_weight,
        proj_bias,
        merge_gain,
        merge_bias,
        fc1_weight.T,
        fc1_bias,
    )
    return vit, hid.T


def solution(mesh):
    return jax.shard_map(
        per_device,
        mesh=mesh,
        in_specs=(
            P(("img", "sp"), None),
            P(None, "img"),
            P(),
            P(),
            P(None, None, "sp"),
            P(),
            P("sp", None),
            P(),
            P(),
            P(),
            P(None, "sp"),
            P("sp"),
        ),
        out_specs=(P(("img", "sp"), None), P("img", "sp")),
        check_vma=False,
    )
```

```python
import math

import jax
import jax.numpy as jnp
from jax import lax
from jax.experimental import pallas as pl
from jax.experimental.pallas import tpu as pltpu
from jax.sharding import PartitionSpec as P

MESH = pl.DeviceIdType.MESH
HEADS = 16
D = 1280
HDIM = 80
PATCHES = 2048
HIDDEN = 5120
SHARE = 320
ROLES = 8
SCALE = math.log2(math.e) / math.sqrt(HDIM)


def norm_rows(v, gain, bias):
    mean = jnp.mean(v, axis=-1, keepdims=True)
    cen = v - mean
    var = jnp.mean(cen * cen, axis=-1, keepdims=True)
    return cen * lax.rsqrt(var + 1e-06) * gain + bias


def kernel(
    x_hbm, pos_hbm, g1_hbm, b1_hbm, wq_hbm, bq_hbm, wp_hbm, pb_hbm, g2_hbm, b2_hbm, fc_hbm, fb_hbm,
    vit_ref, hid_ref, x_ref, pos_ref, g1_ref, b1_ref, bq_ref, pb_ref, g2_ref, b2_ref, fb_ref,
    gat, blk, wg, att, osend, qt, kk, vt, sc, fcv, wqv, bcol, fcol, zf,
    ssend, srecv, precv, wsrecv, wprecv, asem, local,
):
    me = lax.axis_index("sp")
    img, images = lax.axis_index("img"), lax.axis_size("img")
    core = me % 2
    mx = (me // 2) % 4
    my = me // 8

    def dev(dx, dy, p):
        return ((my + dy) % 2) * 8 + ((mx + dx) % 4) * 2 + (core + p) % 2

    barrier = pltpu.get_barrier_semaphore()
    for near in (dev(1, 0, 0), dev(-1, 0, 0), dev(0, 1, 0), dev(0, 0, 1)):
        pl.semaphore_signal(barrier, inc=1, device_id={"img": img, "sp": near}, device_id_type=MESH)
    pl.semaphore_signal(barrier, inc=1, device_id={"img": (img + images // 2) % images, "sp": dev(0, 1, 0)}, device_id_type=MESH)

    loads = [
        (x_hbm, x_ref), (g1_hbm, g1_ref), (b1_hbm, b1_ref), (wp_hbm, wg.at[0, 0]), (bq_hbm, bq_ref), (fb_hbm, fb_ref),
        (wq_hbm, wqv), (pos_hbm, pos_ref), (pb_hbm, pb_ref), (g2_hbm, g2_ref), (b2_hbm, b2_ref), (fc_hbm, fcv),
    ]
    loads = [pltpu.make_async_copy(src, dst, local.at[i]) for i, (src, dst) in enumerate(loads)]
    for load in loads:
        load.start()
    for load in loads[:3]:
        load.wait()

    ln_scope = jax.named_scope("s_ln")
    ln_scope.__enter__()
    xf = x_ref[...].astype(jnp.float32)
    normed = norm_rows(xf, g1_ref[...].reshape(1, D), b1_ref[...].reshape(1, D)).astype(jnp.bfloat16)
    gat[0, 0] = normed
    ln_scope.__exit__(None, None, None)

    with jax.named_scope("s_bar"):
        pl.semaphore_wait(barrier, 5)

    class Gather:
        def __init__(self, ref, up, down, across, flow, groups, parts, srecv, precv, ssend):
            self.ref, self.up, self.down, self.across, self.flow = ref, up, down, across, flow
            self.groups, self.parts, self.srecv, self.precv, self.ssend = groups, parts, srecv, precv, ssend
            self.rows, self.here, self.sem = 0, {}, {}
            for r in range(1, ROLES):
                for g in groups[r]:
                    for i in g:
                        self.sem[r, i] = len(set(self.sem.values())) if i == g[0] else self.sem[r, g[0]]

        def copy(self, src, dst, size, at, rsem, dx, dy, p, other=False):
            return pltpu.make_async_remote_copy(
                src_ref=self.ref.at[src[0], src[1], pl.ds(at, size)],
                dst_ref=self.ref.at[dst[0], dst[1], pl.ds(at, size)],
                send_sem=self.ssend,
                recv_sem=rsem,
                device_id={"img": (img + images // 2) % images if other else img, "sp": dev(dx, dy, p)},
                device_id_type=MESH,
            )

        def pass_on(self, r, i, dx, dy, other=False):
            role = 4 * ((r // 4 + dy) % 2) + (r % 4 - dx) % 4
            self.copy((r, 0), (role, 0), 16, 16 * i, self.srecv.at[self.sem[role, i]], dx, dy, 0, other).start()
            self.rows += 16

        def share(self, r, part):
            at, size, which = self.parts[part]
            self.copy((r, 0), (r, 1), size, at, self.precv.at[r, which], 0, 0, 1).start()
            self.rows += size

        def wait(self, r, g):
            self.copy((r, 0), (r, 0), 16 * len(g), 16 * g[0], self.srecv.at[self.sem[r, g[0]]], 0, 0, 1).wait_recv()
            assert list(g) in [list(v) for v in self.groups[r]]
            if r in (1, 3) and self.across in g:
                self.pass_on(r, self.across, 0, 1)
            here = self.here.setdefault(r, set())
            for part, (at, size, _) in enumerate(self.parts):
                mine = set(range(at // 16, (at + size) // 16))
                if mine <= here | set(g) and not mine <= here:
                    self.share(r, part)
            here.update(g)

        def wait_partner(self, r, which=0):
            size = sum(v[1] for v in self.parts if v[2] == which)
            at = min(v[0] for v in self.parts if v[2] == which)
            self.copy((r, 1), (r, 1), size, at, self.precv.at[r, which], 0, 0, 1).wait_recv()

        def own(self, lo, hi):
            for a, b in list(zip(self.up + self.down, self.down + self.up))[lo:hi]:
                self.pass_on(0, a, 1, 0)
                self.pass_on(0, b, -1, 0)

        def share_own(self):
            for part in range(len(self.parts)):
                self.share(0, part)

        def begin(self):
            self.own(0, 2)
            for n, c in enumerate(self.flow):
                self.pass_on(0, c, 0, 1)
                if n in (1, 3, 5, 7):
                    self.own(2 + n // 2, 3 + n // 2)
            self.share_own()

        def ring_all(self):
            for n, (i, j) in enumerate(zip(self.up, self.down)):
                self.ring(3, i)
                self.ring(1, j)
                if n in (1, 3):
                    self.own(6 + n // 2, 7 + n // 2)

        def ring(self, r, i):
            self.wait(r, [i])
            self.pass_on(r, i, 1 if r == 3 else -1, 0)

        def cross(self, g):
            self.wait(4, g)
            for i in g:
                if i != self.across:
                    self.pass_on(4, i, 1, 0)
                    self.pass_on(4, i, -1, 0)

        def rest(self):
            for r, done in ((3, self.up), (1, self.down)):
                for g in self.groups[r]:
                    if g[0] not in done:
                        self.wait(r, g)

        def far(self, i):
            self.wait(2, [i])
            self.pass_on(2, i, 0, 1)

        def last(self, g):
            for r in (5, 7, 6):
                self.wait(r, g)

        def drain(self):
            size = self.ref.shape[2]
            assert self.rows == 15 * size
            flat = self.ref.reshape(16 * size, D).at[pl.ds(0, self.rows)]
            pltpu.make_async_remote_copy(
                src_ref=flat, dst_ref=flat, send_sem=self.ssend, recv_sem=self.precv.at[0, 0],
                device_id={"sp": dev(0, 0, 1)}, device_id_type=MESH,
            ).wait_send()

    halves = [[0, 1, 2, 3], [4, 5, 6, 7]]
    pairs = [[0, 1], [2, 3], [4, 5], [6, 7]]
    groups = {
        1: [[2], [3], [6], [7], [0, 1], [4, 5]],
        2: [[i] for i in range(8)],
        3: [[0], [1], [4], [5], [2, 3], [6], [7]],
        4: halves, 5: pairs, 6: pairs, 7: pairs,
    }
    flow = [0, 2, 1, 3, 4, 6, 5, 7]
    big = ([0, 1, 4, 5], [2, 3, 6, 7], 7, flow, groups)
    g1 = Gather(gat, *big, [(32 * j, 32, 0) for j in range(4)], srecv, precv, ssend.at[0])
    g2 = Gather(blk, *big, [(32 * j, 32, j) for j in range(4)], srecv, precv, ssend.at[1])
    whole = [[0, 1, 2, 3, 4]]
    two = [[0, 1, 2], [3, 4]]
    wgroups = {
        1: [[4], [3], [2], [0, 1]],
        2: [[i] for i in range(5)],
        3: [[0], [1], [2], [3, 4]],
        4: whole, 5: two, 6: two, 7: two,
    }
    gw = Gather(wg, [0, 1, 2], [4, 3], None, None, wgroups, [(0, 48, 0), (48, 32, 0)], wsrecv, wprecv, ssend.at[2])

    def w_near(r, g):
        gw.wait(r, g)
        for i in g:
            if i in (gw.up if r == 3 else gw.down):
                gw.pass_on(r, i, 1 if r == 3 else -1, 0)
        for i in g:
            if i in ((0, 1, 2) if r == 3 else (4, 3, 2)):
                gw.pass_on(r, i, 0, 1, r == 3)

    def w_cross():
        gw.wait(4, whole[0])
        for i in (0, 1):
            gw.pass_on(4, i, -1, 0)
        for i in (4, 3):
            gw.pass_on(4, i, 1, 0)

    def w_far(i):
        gw.wait(2, [i])
        gw.pass_on(2, i, 0, 1, i != 0)

    g1.begin()
    loads[3].wait()
    for i in range(5):
        gw.pass_on(0, i, 0, 1, True)
    gw.share_own()

    for load in loads[4:6]:
        load.wait()
    lane = lax.broadcasted_iota(jnp.int32, (HDIM, D), 1)
    sub = lax.broadcasted_iota(jnp.int32, (HDIM, D), 0)
    mine = lane == sub + me * HDIM
    for c in range(3):
        col = jnp.sum(jnp.where(mine, bq_ref[c : c + 1, :], 0.0), axis=1, keepdims=True)
        bcol[c] = jnp.broadcast_to(col, (HDIM, 128))
    same = lax.broadcasted_iota(jnp.int32, (SHARE, SHARE), 0) == lax.broadcasted_iota(
        jnp.int32, (SHARE, SHARE), 1
    )
    col = jnp.sum(jnp.where(same, fb_ref[...].reshape(1, SHARE), 0.0), axis=1, keepdims=True)
    fcol[...] = jnp.broadcast_to(col, (SHARE, 128))

    for load in loads[6:8]:
        load.wait()

    def qkv(r, ps=(0, 1)):
        n = 128 * len(ps)
        rows = gat[r, ps[0] : ps[-1] + 1].reshape(n, D)
        out = lax.dot_general(
            wqv[...], rows, (((1,), (1,)), ((), ())), preferred_element_type=jnp.float32
        )
        at = [pl.multiple_of(dev(r % 4, r // 4, p) * 128, 128) for p in ps]
        prow = jnp.concatenate([pos_ref[0:1, pl.ds(a, 128)] for a in at], axis=1).astype(jnp.float32)
        pcol = jnp.concatenate([pos_ref[1:2, pl.ds(a, 128)] for a in at], axis=1).astype(jnp.float32)
        row = lax.broadcasted_iota(jnp.int32, (40, n), 0)
        power = jnp.where(row < 20, row, row - 20).astype(jnp.float32)
        inv = jnp.exp2(power * (-math.log2(10000.0) / 20.0))
        angle = jnp.where(row < 20, prow, pcol) * inv
        cos, sin = jnp.cos(angle), jnp.sin(angle)

        def turn(v):
            lo, hi = v[:40], v[40:]
            return jnp.concatenate([lo * cos - hi * sin, hi * cos + lo * sin], axis=0)

        bias = [jnp.concatenate([bcol[c]] * len(ps), axis=1) for c in range(3)]
        pad = jnp.zeros((128 - HDIM, n), jnp.float32)
        q = turn(out[0:80] + bias[0])
        k = turn(out[80:160] + bias[1])
        v = out[160:240] + bias[2]
        where = pl.ds(ps[0] * 128, n)
        qt[r, :, where] = jnp.concatenate([q, pad], axis=0).astype(jnp.bfloat16)
        kk[r, where] = jnp.concatenate([k, pad], axis=0).T.astype(jnp.bfloat16)
        vt[r, :, where] = v.astype(jnp.bfloat16)

    with jax.named_scope("a_own"):
        g1.wait_partner(0)
        qkv(0)
    with jax.named_scope("a_ring"):
        g1.ring_all()
    with jax.named_scope("a_cross"):
        g1.cross(halves[0])
    with jax.named_scope("a_far0"):
        for i in flow[:4]:
            g1.far(i)
    with jax.named_scope("a_cross1"):
        g1.cross(halves[1])
    with jax.named_scope("a_far1"):
        for i in flow[4:]:
            g1.far(i)
    with jax.named_scope("a_wbegin"):
        gw.own(0, 5)
    with jax.named_scope("a_rest"):
        g1.rest()
    with jax.named_scope("a_qkv"):
        for n, r in enumerate((3, 1, 4, 2)):
            g1.wait_partner(r)
            qkv(r)
            if n > 0:
                g1.last(pairs[n - 1])
    with jax.named_scope("a_last"):
        g1.last(pairs[3])
    with jax.named_scope("w_ring0"):
        w_near(3, [0])
        w_near(1, [4])
        w_cross()
    with jax.named_scope("a_qkv2"):
        for r in (5, 7, 6):
            qkv(r, (0,))
    with jax.named_scope("w_ring1"):
        w_near(3, [1])
        w_near(1, [3])
    with jax.named_scope("a_qkv3"):
        for r in (5, 7, 6):
            g1.wait_partner(r)
            qkv(r, (1,))
    with jax.named_scope("w_ring2"):
        w_near(3, [2])
        w_near(1, [2])

    def score(r, slot):
        top = None
        for kc in range(ROLES):
            s = jnp.dot(kk[kc], qt[r], preferred_element_type=jnp.float32)
            sc[slot, kc] = s
            m = jnp.max(s.reshape(32, 8, 256), axis=0)
            top = m if top is None else jnp.maximum(top, m)
        return jnp.max(top, axis=0, keepdims=True) * SCALE

    def weigh(r, slot, top):
        total, out = None, None
        for kc in range(ROLES):
            w = jnp.exp2(sc[slot, kc] * SCALE - top)
            s = jnp.sum(w.reshape(32, 8, 256), axis=0)
            o = jnp.dot(vt[kc], w.astype(jnp.bfloat16), preferred_element_type=jnp.float32)
            total = s if total is None else total + s
            out = o if out is None else out + o
        out = (out / jnp.sum(total, axis=0, keepdims=True)).astype(jnp.bfloat16)
        for p in range(2):
            osend[2 * r + p] = out[:, p * 128 : (p + 1) * 128]

    def give(r):
        for p in range(2):
            if r == 0 and p == 0:
                continue
            role = 4 * (r // 4) + (-r % 4) % 4
            pltpu.make_async_remote_copy(
                src_ref=osend.at[2 * r + p],
                dst_ref=att.at[2 * role + p],
                send_sem=asem.at[0],
                recv_sem=asem.at[1],
                device_id={"sp": dev(r % 4, r // 4, p)},
                device_id_type=MESH,
            ).start()

    order = (6, 7, 5, 2, 4, 3, 1, 0)
    top = score(order[0], 0)
    for i, r in enumerate(order):
        if i + 1 < ROLES:
            later = score(order[i + 1], (i + 1) % 2)
        weigh(r, i % 2, top)
        top = later
        if i > 0:
            give(order[i - 1])
        with jax.named_scope(f"w_tile{i}"):
            if i == 1:
                w_near(3, [3, 4])
                w_near(1, [0, 1])
            if i == 3:
                w_far(0)
                w_far(4)
            if i == 4:
                w_far(1)
                w_far(3)
            if i == 5:
                w_far(2)
    with jax.named_scope("t_give"):
        give(order[-1])
        att[0] = osend[0]
    with jax.named_scope("w_last"):
        gw.last(two[0])
        gw.last(two[1])
    with jax.named_scope("w_partner"):
        for r in range(ROLES):
            gw.wait_partner(r)
    with jax.named_scope("t_back"):
        pltpu.make_async_remote_copy(
            src_ref=osend.at[pl.ds(1, 15)], dst_ref=att.at[pl.ds(1, 15)], send_sem=asem.at[0], recv_sem=asem.at[1],
            device_id={"sp": dev(0, 0, 1)}, device_id_type=MESH,
        ).wait_recv()

    for load in loads[8:11]:
        load.wait()
    got = att[...].reshape(D, 128).T
    out = jnp.dot(got, wg[...].reshape(D, D), preferred_element_type=jnp.float32)
    vit = (x_ref[...].astype(jnp.float32) + out + pb_ref[...].reshape(1, D)).astype(jnp.bfloat16)
    vit_ref[...] = vit
    zn = norm_rows(vit.astype(jnp.float32), g2_ref[...].reshape(1, D), b2_ref[...].reshape(1, D))
    for b in range(D // 128):
        zf[b] = zn[:, b * 128 : (b + 1) * 128]
    for j in range(4):
        for b in range(D // 128):
            blk[0, 0, pl.ds(j * 32, 32), pl.ds(b * 128, 128)] = zf[
                b, pl.ds(j, 32, stride=4), :
            ].astype(jnp.bfloat16)

    g2.begin()
    loads[11].wait()

    def fc1(dy, j):
        parts = []
        for ax in range(4):
            r = 4 * dy + (ax + 4 - mx) % 4
            for c in range(2):
                parts.append(blk[r, (c + core) % 2, pl.ds(j * 32, 32)])
        return lax.dot_general(
            fcv[:, j * D : (j + 1) * D],
            jnp.concatenate(parts, axis=0),
            (((1,), (1,)), ((), ())),
            preferred_element_type=jnp.float32,
        )

    def finish(dy, total):
        v = total + jnp.concatenate([fcol[...], fcol[...]], axis=1)
        at = pl.multiple_of(((my + dy) % 2) * 256, 256)
        hid_ref[:, pl.ds(at, 256)] = (0.5 * v * (1.0 + lax.erf(v * (2.0**-0.5)))).astype(jnp.bfloat16)

    with jax.named_scope("b_ring"):
        g2.ring_all()
    with jax.named_scope("b_cross"):
        g2.cross(halves[0])
    with jax.named_scope("b_far0"):
        for i in flow[:4]:
            g2.far(i)
    with jax.named_scope("b_cross1"):
        g2.cross(halves[1])
    with jax.named_scope("b_far1"):
        for i in flow[4:]:
            g2.far(i)
    with jax.named_scope("b_rest"):
        g2.rest()
    def partner(j):
        with jax.named_scope(f"b_partner{j}"):
            for r in (5, 7, 6):
                g2.wait_partner(r, j)

    with jax.named_scope("b_last0"):
        g2.last(pairs[0])
    with jax.named_scope("b_far_p"):
        for r in (0, 3, 1, 2, 4):
            for j in range(4):
                g2.wait_partner(r, j)
    with jax.named_scope("b_fc1_a"):
        total = fc1(0, 0) + fc1(0, 1)
    with jax.named_scope("b_last1"):
        g2.last(pairs[1])
    with jax.named_scope("b_fc1_b"):
        finish(0, total + fc1(0, 2) + fc1(0, 3))
    partner(0)
    with jax.named_scope("b_fc1_c"):
        total = fc1(1, 0)
    with jax.named_scope("b_last2"):
        g2.last(pairs[2])
    with jax.named_scope("b_last3"):
        g2.last(pairs[3])
    partner(1)
    with jax.named_scope("b_fc1_d"):
        total = total + fc1(1, 1)
    partner(2)
    with jax.named_scope("b_fc1_e"):
        total = total + fc1(1, 2)
    partner(3)
    with jax.named_scope("b_fc1_f"):
        finish(1, total + fc1(1, 3))

    with jax.named_scope("drain"):
        for g in (g1, gw, g2):
            g.drain()
        pltpu.make_async_remote_copy(
            src_ref=osend.at[pl.ds(1, 15)], dst_ref=att.at[pl.ds(1, 15)], send_sem=asem.at[0], recv_sem=asem.at[1],
            device_id={"sp": dev(0, 0, 1)}, device_id_type=MESH,
        ).wait_send()


def per_device(
    patches, pos_ids, norm_gain, norm_bias, qkv_weight, qkv_bias, proj_weight, proj_bias, merge_gain, merge_bias,
    fc1_weight, fc1_bias,
):
    vmem = pl.BlockSpec(memory_space=pltpu.VMEM)
    hbm = pl.BlockSpec(memory_space=pl.ANY)
    bf, f32 = jnp.bfloat16, jnp.float32
    dma = pltpu.SemaphoreType.DMA
    vit, hid = pl.pallas_call(
        kernel,
        out_shape=(pltpu.VMEM((128, D), bf), pltpu.VMEM((SHARE, 512), bf)),
        in_specs=[hbm] * 12,
        out_specs=(vmem, vmem),
        scratch_shapes=[
            pltpu.VMEM((128, D), bf),
            pltpu.VMEM((2, PATCHES), jnp.int32),
            pltpu.VMEM((D,), f32),
            pltpu.VMEM((D,), f32),
            pltpu.VMEM((3, D), f32),
            pltpu.VMEM((D,), f32),
            pltpu.VMEM((D,), f32),
            pltpu.VMEM((D,), f32),
            pltpu.VMEM((SHARE,), f32),
            pltpu.VMEM((ROLES, 2, 128, D), bf),
            pltpu.VMEM((ROLES, 2, 128, D), bf),
            pltpu.VMEM((ROLES, 2, HDIM, D), bf),
            pltpu.VMEM((2 * ROLES, HDIM, 128), bf),
            pltpu.VMEM((2 * ROLES, HDIM, 128), bf),
            pltpu.VMEM((ROLES, 128, 256), bf),
            pltpu.VMEM((ROLES, 256, 128), bf),
            pltpu.VMEM((ROLES, HDIM, 256), bf),
            pltpu.VMEM((2, ROLES, 256, 256), f32),
            pltpu.VMEM((SHARE, HIDDEN), bf),
            pltpu.VMEM((3 * HDIM, D), bf),
            pltpu.VMEM((3, HDIM, 128), f32),
            pltpu.VMEM((SHARE, 128), f32),
            pltpu.VMEM((D // 128, 128, 128), f32),
            dma((3,)),
            dma((35,)),
            dma((ROLES, 4)),
            dma((20,)),
            dma((ROLES, 1)),
            dma((2,)),
            dma((12,)),
        ],
        compiler_params=pltpu.CompilerParams(
            collective_id=0, has_side_effects=True, vmem_limit_bytes=58 * 1024 * 1024
        ),
    )(
        patches,
        pos_ids,
        norm_gain,
        norm_bias,
        qkv_weight.transpose(1, 2, 0).reshape(3 * HDIM, D),
        qkv_bias,
        proj_weight,
        proj_bias,
        merge_gain,
        merge_bias,
        fc1_weight.T,
        fc1_bias,
    )
    return vit, hid.T


def solution(mesh):
    return jax.shard_map(
        per_device,
        mesh=mesh,
        in_specs=(
            P(("img", "sp"), None),
            P(None, "img"),
            P(),
            P(),
            P(None, None, "sp"),
            P(),
            P("sp", None),
            P(),
            P(),
            P(),
            P(None, "sp"),
            P("sp"),
        ),
        out_specs=(P(("img", "sp"), None), P("img", "sp")),
        check_vma=False,
    )
```

```python
import math

import jax
import jax.numpy as jnp
from jax import lax
from jax.experimental import pallas as pl
from jax.experimental.pallas import tpu as pltpu
from jax.sharding import PartitionSpec as P

MESH = pl.DeviceIdType.MESH
HEADS = 16
D = 1280
HDIM = 80
PATCHES = 2048
HIDDEN = 5120
SHARE = 320
ROLES = 8
SCALE = math.log2(math.e) / math.sqrt(HDIM)


def norm_rows(v, gain, bias):
    mean = jnp.mean(v, axis=-1, keepdims=True)
    cen = v - mean
    var = jnp.mean(cen * cen, axis=-1, keepdims=True)
    return cen * lax.rsqrt(var + 1e-06) * gain + bias


def kernel(
    x_hbm, pos_hbm, g1_hbm, b1_hbm, wq_hbm, bq_hbm, wp_hbm, pb_hbm, g2_hbm, b2_hbm, fc_hbm, fb_hbm,
    vit_ref, hid_ref, x_ref, pos_ref, g1_ref, b1_ref, bq_ref, pb_ref, g2_ref, b2_ref, fb_ref,
    gat, blk, wg, att, osend, qt, kk, vt, sc, fcv, wqv, bcol, fcol, zf, acc, osum, stat,
    ssend, srecv, precv, wsrecv, wprecv, asem, local,
):
    me = lax.axis_index("sp")
    img, images = lax.axis_index("img"), lax.axis_size("img")
    core = me % 2
    mx = (me // 2) % 4
    my = me // 8

    def dev(dx, dy, p):
        return ((my + dy) % 2) * 8 + ((mx + dx) % 4) * 2 + (core + p) % 2

    barrier = pltpu.get_barrier_semaphore()
    for near in (dev(1, 0, 0), dev(-1, 0, 0), dev(0, 1, 0), dev(0, 0, 1)):
        pl.semaphore_signal(barrier, inc=1, device_id={"img": img, "sp": near}, device_id_type=MESH)
    pl.semaphore_signal(barrier, inc=1, device_id={"img": (img + images // 2) % images, "sp": dev(0, 1, 0)}, device_id_type=MESH)

    loads = [
        (x_hbm, x_ref), (g1_hbm, g1_ref), (b1_hbm, b1_ref), (wp_hbm, wg.at[0, 0]), (bq_hbm, bq_ref), (fb_hbm, fb_ref),
        (wq_hbm, wqv), (pos_hbm, pos_ref), (pb_hbm, pb_ref), (g2_hbm, g2_ref), (b2_hbm, b2_ref), (fc_hbm, fcv),
    ]
    loads = [pltpu.make_async_copy(src, dst, local.at[i]) for i, (src, dst) in enumerate(loads)]
    for load in loads:
        load.start()
    with jax.named_scope("s_load"):
        for load in loads[:3]:
            load.wait()

    ln_scope = jax.named_scope("s_ln")
    ln_scope.__enter__()
    xf = x_ref[...].astype(jnp.float32)
    normed = norm_rows(xf, g1_ref[...].reshape(1, D), b1_ref[...].reshape(1, D)).astype(jnp.bfloat16)
    gat[0, 0] = normed
    ln_scope.__exit__(None, None, None)

    with jax.named_scope("s_bar"):
        pl.semaphore_wait(barrier, 5)

    class Gather:
        def __init__(self, ref, up, down, across, flow, groups, parts, srecv, precv, ssend):
            self.ref, self.up, self.down, self.across, self.flow = ref, up, down, across, flow
            self.groups, self.parts, self.srecv, self.precv, self.ssend = groups, parts, srecv, precv, ssend
            self.rows, self.here, self.sem = 0, {}, {}
            for r in range(1, ROLES):
                for g in groups[r]:
                    for i in g:
                        self.sem[r, i] = len(set(self.sem.values())) if i == g[0] else self.sem[r, g[0]]

        def copy(self, src, dst, size, at, rsem, dx, dy, p, other=False):
            return pltpu.make_async_remote_copy(
                src_ref=self.ref.at[src[0], src[1], pl.ds(at, size)],
                dst_ref=self.ref.at[dst[0], dst[1], pl.ds(at, size)],
                send_sem=self.ssend,
                recv_sem=rsem,
                device_id={"img": (img + images // 2) % images if other else img, "sp": dev(dx, dy, p)},
                device_id_type=MESH,
            )

        def pass_on(self, r, i, dx, dy, other=False):
            role = 4 * ((r // 4 + dy) % 2) + (r % 4 - dx) % 4
            self.copy((r, 0), (role, 0), 16, 16 * i, self.srecv.at[self.sem[role, i]], dx, dy, 0, other).start()
            self.rows += 16

        def which(self, r, which):
            return which if r in (5, 6, 7) else 0

        def slot(self, r, which):
            return 0 if self.precv is wprecv else (3 * (r - 5) + which - 1 + ROLES if which else r)

        def share(self, r, part):
            at, size, which = self.parts[part]
            which = self.which(r, which)
            self.copy((r, 0), (r, 1), size, at, self.precv.at[self.slot(r, which)], 0, 0, 1).start()
            self.rows += size

        def wait(self, r, g):
            self.copy((r, 0), (r, 0), 16 * len(g), 16 * g[0], self.srecv.at[self.sem[r, g[0]]], 0, 0, 1).wait_recv()
            assert list(g) in [list(v) for v in self.groups[r]]
            if r in (1, 3) and self.across in g:
                self.pass_on(r, self.across, 0, 1)
            here = self.here.setdefault(r, set())
            for part, (at, size, _) in enumerate(self.parts):
                mine = set(range(at // 16, (at + size) // 16))
                if mine <= here | set(g) and not mine <= here:
                    self.share(r, part)
            here.update(g)

        def wait_partner(self, r, which=0):
            size = sum(v[1] for v in self.parts if self.which(r, v[2]) == which)
            at = min(v[0] for v in self.parts if self.which(r, v[2]) == which)
            self.copy((r, 1), (r, 1), size, at, self.precv.at[self.slot(r, which)], 0, 0, 1).wait_recv()

        def own(self, lo, hi):
            for a, b in list(zip(self.up + self.down, self.down + self.up))[lo:hi]:
                self.pass_on(0, a, 1, 0)
                self.pass_on(0, b, -1, 0)

        def share_own(self):
            for part in range(len(self.parts)):
                self.share(0, part)

        def begin(self):
            self.own(0, 2)
            for n, c in enumerate(self.flow):
                self.pass_on(0, c, 0, 1)
                if n in (1, 3, 5, 7):
                    self.own(2 + n // 2, 3 + n // 2)
            self.share_own()

        def ring_all(self):
            for n, (i, j) in enumerate(zip(self.up, self.down)):
                self.ring(3, i)
                self.ring(1, j)
                if n in (1, 3):
                    self.own(6 + n // 2, 7 + n // 2)

        def ring(self, r, i):
            self.wait(r, [i])
            self.pass_on(r, i, 1 if r == 3 else -1, 0)

        def cross(self, g):
            self.wait(4, g)
            for i in g:
                if i != self.across:
                    self.pass_on(4, i, 1, 0)
                    self.pass_on(4, i, -1, 0)

        def rest(self):
            for r, done in ((3, self.up), (1, self.down)):
                for g in self.groups[r]:
                    if g[0] not in done:
                        self.wait(r, g)

        def far(self, i):
            self.wait(2, [i])
            self.pass_on(2, i, 0, 1)

        def last(self, g):
            for r in (5, 7, 6):
                self.wait(r, g)

        def drain(self):
            size = self.ref.shape[2]
            assert self.rows == 15 * size
            flat = self.ref.reshape(16 * size, D).at[pl.ds(0, self.rows)]
            pltpu.make_async_remote_copy(
                src_ref=flat, dst_ref=flat, send_sem=self.ssend, recv_sem=self.precv.at[0],
                device_id={"sp": dev(0, 0, 1)}, device_id_type=MESH,
            ).wait_send()

    halves = [[0, 1, 2, 3], [4, 5, 6, 7]]
    pairs = [[0, 1], [2, 3], [4, 5], [6, 7]]
    groups = {
        1: [[2], [3], [6], [7], [0, 1], [4, 5]],
        2: [[i] for i in range(8)],
        3: [[0], [1], [4], [5], [2, 3], [6], [7]],
        4: halves, 5: pairs, 6: pairs, 7: pairs,
    }
    flow = [0, 2, 1, 3, 4, 6, 5, 7]
    big = ([0, 1, 4, 5], [2, 3, 6, 7], 7, flow, groups)
    g1 = Gather(gat, *big, [(32 * j, 32, 0) for j in range(4)], srecv, precv, ssend.at[0])
    g2 = Gather(blk, *big, [(32 * j, 32, j) for j in range(4)], srecv, precv, ssend.at[1])
    whole = [[0, 1, 2, 3, 4]]
    two = [[0, 1, 2], [3, 4]]
    wgroups = {
        1: [[4], [3], [2], [0, 1]],
        2: [[i] for i in range(5)],
        3: [[0], [1], [2], [3, 4]],
        4: whole, 5: two, 6: two, 7: two,
    }
    gw = Gather(wg, [0, 1, 2], [4, 3], None, None, wgroups, [(0, 48, 0), (48, 32, 0)], wsrecv, wprecv, ssend.at[2])

    def w_near(r, g):
        gw.wait(r, g)
        for i in g:
            if i in (gw.up if r == 3 else gw.down):
                gw.pass_on(r, i, 1 if r == 3 else -1, 0)
        for i in g:
            if i != (4 if r == 3 else 0):
                gw.pass_on(r, i, 0, 1, r == 3)

    def w_cross():
        gw.wait(4, whole[0])
        gw.pass_on(4, 0, -1, 0)
        gw.pass_on(4, 4, 1, 0)

    def w_far(i):
        gw.wait(2, [i])
        gw.pass_on(2, i, 0, 1, i != 0)

    g1.begin()
    loads[3].wait()
    for i in range(5):
        gw.pass_on(0, i, 0, 1, True)
    gw.share_own()

    for load in loads[4:6]:
        load.wait()
    lane = lax.broadcasted_iota(jnp.int32, (HDIM, D), 1)
    sub = lax.broadcasted_iota(jnp.int32, (HDIM, D), 0)
    mine = lane == sub + me * HDIM
    for c in range(3):
        col = jnp.sum(jnp.where(mine, bq_ref[c : c + 1, :], 0.0), axis=1, keepdims=True)
        bcol[c] = jnp.broadcast_to(col, (HDIM, 128))
    same = lax.broadcasted_iota(jnp.int32, (SHARE, SHARE), 0) == lax.broadcasted_iota(
        jnp.int32, (SHARE, SHARE), 1
    )
    col = jnp.sum(jnp.where(same, fb_ref[...].reshape(1, SHARE), 0.0), axis=1, keepdims=True)
    fcol[...] = jnp.broadcast_to(col, (SHARE, 128))

    for load in loads[6:8]:
        load.wait()

    def qkv(r, ps=(0, 1)):
        n = 128 * len(ps)
        rows = gat[r, ps[0] : ps[-1] + 1].reshape(n, D)
        out = lax.dot_general(
            wqv[...], rows, (((1,), (1,)), ((), ())), preferred_element_type=jnp.float32
        )
        at = [pl.multiple_of(dev(r % 4, r // 4, p) * 128, 128) for p in ps]
        prow = jnp.concatenate([pos_ref[0:1, pl.ds(a, 128)] for a in at], axis=1).astype(jnp.float32)
        pcol = jnp.concatenate([pos_ref[1:2, pl.ds(a, 128)] for a in at], axis=1).astype(jnp.float32)
        row = lax.broadcasted_iota(jnp.int32, (40, n), 0)
        power = jnp.where(row < 20, row, row - 20).astype(jnp.float32)
        inv = jnp.exp2(power * (-math.log2(10000.0) / 20.0))
        angle = jnp.where(row < 20, prow, pcol) * inv
        cos, sin = jnp.cos(angle), jnp.sin(angle)

        def turn(v):
            lo, hi = v[:40], v[40:]
            return jnp.concatenate([lo * cos - hi * sin, hi * cos + lo * sin], axis=0)

        bias = [jnp.concatenate([bcol[c]] * len(ps), axis=1) for c in range(3)]
        pad = jnp.zeros((128 - HDIM, n), jnp.float32)
        q = turn(out[0:80] + bias[0])
        k = turn(out[80:160] + bias[1])
        v = out[160:240] + bias[2]
        where = pl.ds(ps[0] * 128, n)
        qt[r, :, where] = jnp.concatenate([q, pad], axis=0).astype(jnp.bfloat16)
        kk[r, where] = jnp.concatenate([k, pad], axis=0).T.astype(jnp.bfloat16)
        vt[r, :, where] = v.astype(jnp.bfloat16)

    early, late = (0, 3, 1, 4, 2), (5, 7, 6)

    def score(r, slot, keys):
        top = None
        for n, c in enumerate(keys):
            s = jnp.dot(kk[c], qt[r], preferred_element_type=jnp.float32)
            sc[slot, n] = s
            m = jnp.max(s.reshape(32, 8, 256), axis=0)
            top = m if top is None else jnp.maximum(top, m)
        return jnp.max(top, axis=0, keepdims=True) * SCALE

    def weigh(slot, keys, top):
        total, out = None, None
        for n, c in enumerate(keys):
            w = jnp.exp2(sc[slot, n] * SCALE - top)
            s = jnp.sum(w.reshape(32, 8, 256), axis=0)
            o = jnp.dot(vt[c], w.astype(jnp.bfloat16), preferred_element_type=jnp.float32)
            total = s if total is None else total + s
            out = o if out is None else out + o
        return jnp.sum(total, axis=0, keepdims=True), out

    def begin_tile(n, top):
        later = score(early[n + 1], (n + 1) % 2, early) if n < 4 else None
        total, out = weigh(n % 2, early, top)
        osum[n] = out
        stat[n, 0:1] = top
        stat[n, 1:2] = total
        return later

    def end_tile(r, slot, top):
        if r in early:
            n = early.index(r)
            before = stat[n, 0:1]
            both = jnp.maximum(before, top)
            total, out = weigh(slot, late, both)
            old = jnp.exp2(before - both)
            total, out = total + stat[n, 1:2] * old, out + osum[n] * old
        else:
            total, out = weigh(slot, early + late, top)
        out = (out / total).astype(jnp.bfloat16)
        for p in range(2):
            osend[2 * r + p] = out[:, p * 128 : (p + 1) * 128]

    with jax.named_scope("a_own"):
        g1.wait_partner(0)
        qkv(0)
    with jax.named_scope("a_ring"):
        g1.ring_all()
    with jax.named_scope("a_cross"):
        g1.cross(halves[0])
    with jax.named_scope("a_far0"):
        for i in flow[:4]:
            g1.far(i)
    with jax.named_scope("a_cross1"):
        g1.cross(halves[1])
    with jax.named_scope("a_far1"):
        for i in flow[4:]:
            g1.far(i)
    with jax.named_scope("a_wbegin"):
        gw.own(0, 5)
    with jax.named_scope("a_rest"):
        g1.rest()
    with jax.named_scope("a_qkv"):
        for r in (3, 1, 4, 2):
            g1.wait_partner(r)
            qkv(r)
    with jax.named_scope("a_early0"):
        top = score(early[0], 0, early)
    with jax.named_scope("a_last0"):
        g1.last(pairs[0])
    with jax.named_scope("a_early1"):
        top = begin_tile(0, top)
        top = begin_tile(1, top)
    with jax.named_scope("a_last1"):
        g1.last(pairs[1])
    with jax.named_scope("a_early2"):
        top = begin_tile(2, top)
        top = begin_tile(3, top)
    with jax.named_scope("a_last2"):
        g1.last(pairs[2])
    with jax.named_scope("a_early3"):
        begin_tile(4, top)
    with jax.named_scope("a_last"):
        g1.last(pairs[3])
    with jax.named_scope("a_qkv2"):
        for r in (5, 7, 6):
            qkv(r, (0,))
    with jax.named_scope("w_ring0"):
        w_near(3, [0])
        w_near(1, [4])
    with jax.named_scope("a_qkv3"):
        for n, r in enumerate((5, 7, 6)):
            g1.wait_partner(r)
            qkv(r, (1,))
            if n == 1:
                w_near(3, [1])
                w_near(1, [3])
    with jax.named_scope("w_ring1"):
        w_near(3, [2])
        w_near(1, [2])
        w_cross()

    def give(r):
        for p in range(2):
            if r == 0 and p == 0:
                continue
            role = 4 * (r // 4) + (-r % 4) % 4
            pltpu.make_async_remote_copy(
                src_ref=osend.at[2 * r + p],
                dst_ref=att.at[2 * role + p],
                send_sem=asem.at[0],
                recv_sem=asem.at[1],
                device_id={"sp": dev(r % 4, r // 4, p)},
                device_id_type=MESH,
            ).start()

    order = (6, 7, 5, 2, 4, 3, 1, 0)
    def keys(r):
        return late if r in early else early + late

    top = score(order[0], 0, keys(order[0]))
    for i, r in enumerate(order):
        if i + 1 < ROLES:
            later = score(order[i + 1], (i + 1) % 2, keys(order[i + 1]))
        end_tile(r, i % 2, top)
        top = later
        if i > 0:
            give(order[i - 1])
        with jax.named_scope(f"w_tile{i}"):
            if i == 0:
                w_near(3, [3, 4])
                w_near(1, [0, 1])
            if i == 2:
                w_far(0)
                w_far(4)
            if i == 4:
                w_far(1)
                w_far(3)
    with jax.named_scope("t_give"):
        give(order[-1])
        att[0] = osend[0]
    with jax.named_scope("w_far"):
        w_far(2)
    with jax.named_scope("w_last"):
        gw.last(two[0])
        gw.last(two[1])
    with jax.named_scope("w_partner"):
        pltpu.make_async_remote_copy(
            src_ref=wg.at[:, 1], dst_ref=wg.at[:, 1], send_sem=ssend.at[2], recv_sem=wprecv.at[0],
            device_id={"img": img, "sp": dev(0, 0, 1)}, device_id_type=MESH,
        ).wait_recv()
    with jax.named_scope("t_back"):
        pltpu.make_async_remote_copy(
            src_ref=osend.at[pl.ds(1, 15)], dst_ref=att.at[pl.ds(1, 15)], send_sem=asem.at[0], recv_sem=asem.at[1],
            device_id={"sp": dev(0, 0, 1)}, device_id_type=MESH,
        ).wait_recv()

    for load in loads[8:11]:
        load.wait()
    got = att[...].reshape(D, 128).T
    out = jnp.dot(got, wg[...].reshape(D, D), preferred_element_type=jnp.float32)
    vit = (x_ref[...].astype(jnp.float32) + out + pb_ref[...].reshape(1, D)).astype(jnp.bfloat16)
    vit_ref[...] = vit
    zn = norm_rows(vit.astype(jnp.float32), g2_ref[...].reshape(1, D), b2_ref[...].reshape(1, D))
    for b in range(D // 128):
        zf[b] = zn[:, b * 128 : (b + 1) * 128]
    for j in range(4):
        for b in range(D // 128):
            blk[0, 0, pl.ds(j * 32, 32), pl.ds(b * 128, 128)] = zf[
                b, pl.ds(j, 32, stride=4), :
            ].astype(jnp.bfloat16)

    g2.begin()
    loads[11].wait()

    def fc1(dy, j):
        parts = []
        for ax in range(4):
            r = 4 * dy + (ax + 4 - mx) % 4
            for c in range(2):
                parts.append(blk[r, (c + core) % 2, pl.ds(j * 32, 32)])
        return lax.dot_general(
            fcv[:, j * D : (j + 1) * D],
            jnp.concatenate(parts, axis=0),
            (((1,), (1,)), ((), ())),
            preferred_element_type=jnp.float32,
        )

    def finish(dy, total):
        v = total + jnp.concatenate([fcol[...], fcol[...]], axis=1)
        at = pl.multiple_of(((my + dy) % 2) * 256, 256)
        hid_ref[:, pl.ds(at, 256)] = (0.5 * v * (1.0 + lax.erf(v * (2.0**-0.5)))).astype(jnp.bfloat16)

    with jax.named_scope("b_ring"):
        g2.ring_all()
    with jax.named_scope("b_cross"):
        g2.cross(halves[0])
    with jax.named_scope("b_far0"):
        for i in flow[:4]:
            g2.far(i)
    with jax.named_scope("b_cross1"):
        g2.cross(halves[1])
    with jax.named_scope("b_far1"):
        for i in flow[4:]:
            g2.far(i)
    with jax.named_scope("b_rest"):
        g2.rest()
    def partner(j):
        with jax.named_scope(f"b_partner{j}"):
            for r in (5, 7, 6):
                g2.wait_partner(r, j)

    with jax.named_scope("b_last0"):
        g2.last(pairs[0])
    with jax.named_scope("b_far_p"):
        for r in (0, 3, 1, 2, 4):
            g2.wait_partner(r)
    with jax.named_scope("b_fc1_a"):
        acc[...] = fc1(0, 0) + fc1(0, 1)
    with jax.named_scope("b_last1"):
        g2.last(pairs[1])
    with jax.named_scope("b_fc1_b"):
        finish(0, acc[...] + fc1(0, 2) + fc1(0, 3))
    partner(0)
    with jax.named_scope("b_fc1_c"):
        acc[...] = fc1(1, 0)
    partner(1)
    with jax.named_scope("b_fc1_d"):
        acc[...] += fc1(1, 1)
    with jax.named_scope("b_last2"):
        g2.last(pairs[2])
    with jax.named_scope("b_last3"):
        g2.last(pairs[3])
    partner(2)
    with jax.named_scope("b_fc1_e"):
        acc[...] += fc1(1, 2)
    partner(3)
    with jax.named_scope("b_fc1_f"):
        finish(1, acc[...] + fc1(1, 3))

    with jax.named_scope("drain"):
        for g in (g1, gw, g2):
            g.drain()
        pltpu.make_async_remote_copy(
            src_ref=osend.at[pl.ds(1, 15)], dst_ref=att.at[pl.ds(1, 15)], send_sem=asem.at[0], recv_sem=asem.at[1],
            device_id={"sp": dev(0, 0, 1)}, device_id_type=MESH,
        ).wait_send()


def put(vit_ref, hid_ref, vit_hbm, hid_hbm, sem):
    copies = [
        pltpu.make_async_copy(vit_ref, vit_hbm, sem.at[0]),
        pltpu.make_async_copy(hid_ref, hid_hbm, sem.at[1]),
    ]
    for copy in copies:
        copy.start()
    for copy in copies:
        copy.wait()


def per_device(
    patches, pos_ids, norm_gain, norm_bias, qkv_weight, qkv_bias, proj_weight, proj_bias, merge_gain, merge_bias,
    fc1_weight, fc1_bias,
):
    vmem = pl.BlockSpec(memory_space=pltpu.VMEM)
    hbm = pl.BlockSpec(memory_space=pl.ANY)
    bf, f32 = jnp.bfloat16, jnp.float32
    dma = pltpu.SemaphoreType.DMA
    vit, hid = pl.pallas_call(
        kernel,
        out_shape=(pltpu.VMEM((128, D), bf), pltpu.VMEM((SHARE, 512), bf)),
        in_specs=[hbm] * 12,
        out_specs=(vmem, vmem),
        scratch_shapes=[
            pltpu.VMEM((128, D), bf),
            pltpu.VMEM((2, PATCHES), jnp.int32),
            pltpu.VMEM((D,), f32),
            pltpu.VMEM((D,), f32),
            pltpu.VMEM((3, D), f32),
            pltpu.VMEM((D,), f32),
            pltpu.VMEM((D,), f32),
            pltpu.VMEM((D,), f32),
            pltpu.VMEM((SHARE,), f32),
            pltpu.VMEM((ROLES, 2, 128, D), bf),
            pltpu.VMEM((ROLES, 2, 128, D), bf),
            pltpu.VMEM((ROLES, 2, HDIM, D), bf),
            pltpu.VMEM((2 * ROLES, HDIM, 128), bf),
            pltpu.VMEM((2 * ROLES, HDIM, 128), bf),
            pltpu.VMEM((ROLES, 128, 256), bf),
            pltpu.VMEM((ROLES, 256, 128), bf),
            pltpu.VMEM((ROLES, HDIM, 256), bf),
            pltpu.VMEM((2, ROLES, 256, 256), f32),
            pltpu.VMEM((SHARE, HIDDEN), bf),
            pltpu.VMEM((3 * HDIM, D), bf),
            pltpu.VMEM((3, HDIM, 128), f32),
            pltpu.VMEM((SHARE, 128), f32),
            pltpu.VMEM((D // 128, 128, 128), f32),
            pltpu.VMEM((SHARE, 256), f32),
            pltpu.VMEM((5, HDIM, 256), f32),
            pltpu.VMEM((5, 8, 256), f32),
            dma((3,)),
            dma((35,)),
            dma((ROLES + 9,)),
            dma((20,)),
            dma((1,)),
            dma((2,)),
            dma((12,)),
        ],
        compiler_params=pltpu.CompilerParams(
            collective_id=0, has_side_effects=True, vmem_limit_bytes=58 * 1024 * 1024
        ),
    )(
        patches,
        pos_ids,
        norm_gain,
        norm_bias,
        qkv_weight.transpose(1, 2, 0).reshape(3 * HDIM, D),
        qkv_bias,
        proj_weight,
        proj_bias,
        merge_gain,
        merge_bias,
        fc1_weight.T,
        fc1_bias,
    )
    vit, hid = pl.pallas_call(
        put,
        out_shape=(jax.ShapeDtypeStruct((128, D), bf), jax.ShapeDtypeStruct((SHARE, 512), bf)),
        in_specs=[vmem, vmem],
        out_specs=(hbm, hbm),
        scratch_shapes=[dma((2,))],
    )(pltpu.with_memory_space_constraint(vit, pltpu.VMEM), pltpu.with_memory_space_constraint(hid, pltpu.VMEM))
    return vit, hid.T


def solution(mesh):
    return jax.shard_map(
        per_device,
        mesh=mesh,
        in_specs=(
            P(("img", "sp"), None),
            P(None, "img"),
            P(),
            P(),
            P(None, None, "sp"),
            P(),
            P("sp", None),
            P(),
            P(),
            P(),
            P(None, "sp"),
            P("sp"),
        ),
        out_specs=(P(("img", "sp"), None), P("img", "sp")),
        check_vma=False,
    )
```

```python
import math

import jax
import jax.numpy as jnp
from jax import lax
from jax.experimental import pallas as pl
from jax.experimental.pallas import tpu as pltpu
from jax.sharding import PartitionSpec as P

MESH = pl.DeviceIdType.MESH
HEADS = 16
D = 1280
HDIM = 80
PATCHES = 2048
HIDDEN = 5120
SHARE = 320
ROLES = 8
SCALE = math.log2(math.e) / math.sqrt(HDIM)


def norm_rows(v, gain, bias):
    mean = jnp.mean(v, axis=-1, keepdims=True)
    cen = v - mean
    var = jnp.mean(cen * cen, axis=-1, keepdims=True)
    return cen * lax.rsqrt(var + 1e-06) * gain + bias


def kernel(
    x_hbm, pos_hbm, g1_hbm, b1_hbm, wq_hbm, bq_hbm, wp_hbm, pb_hbm, g2_hbm, b2_hbm, fc_hbm, fb_hbm,
    vit_ref, hid_ref, x_ref, pos_ref, g1_ref, b1_ref, bq_ref, pb_ref, g2_ref, b2_ref, fb_ref,
    gat, blk, wg, att, osend, qt, kk, vt, sc, fcv, wqv, bcol, fcol, zf, acc, osum, stat,
    wqo, trig, stage, kin, ssend, nrecv, nprecv, srecv, precv, wsrecv, wprecv, hsend, hrecv, asem, local,
):
    me = lax.axis_index("sp")
    img, images = lax.axis_index("img"), lax.axis_size("img")
    core = me % 2
    mx = (me // 2) % 4
    my = me // 8

    def dev(dx, dy, p):
        return ((my + dy) % 2) * 8 + ((mx + dx) % 4) * 2 + (core + p) % 2

    barrier = pltpu.get_barrier_semaphore()
    for near in (dev(1, 0, 0), dev(-1, 0, 0), dev(0, 1, 0), dev(0, 0, 1)):
        pl.semaphore_signal(barrier, inc=1, device_id={"img": img, "sp": near}, device_id_type=MESH)
    pl.semaphore_signal(barrier, inc=1, device_id={"img": (img + images // 2) % images, "sp": dev(0, 1, 0)}, device_id_type=MESH)

    loads = [
        (x_hbm, x_ref), (g1_hbm, g1_ref), (b1_hbm, b1_ref), (wq_hbm, wqv), (wp_hbm, wg.at[0, 0]), (bq_hbm, bq_ref),
        (fb_hbm, fb_ref), (pos_hbm, pos_ref), (pb_hbm, pb_ref), (g2_hbm, g2_ref), (b2_hbm, b2_ref), (fc_hbm, fcv),
    ]
    loads = [pltpu.make_async_copy(src, dst, local.at[i]) for i, (src, dst) in enumerate(loads)]
    for load in loads:
        load.start()
    with jax.named_scope("s_load"):
        for load in loads[:3]:
            load.wait()

    ln_scope = jax.named_scope("s_ln")
    ln_scope.__enter__()
    xf = x_ref[...].astype(jnp.float32)
    normed = norm_rows(xf, g1_ref[...].reshape(1, D), b1_ref[...].reshape(1, D)).astype(jnp.bfloat16)
    gat[0, 0] = normed
    ln_scope.__exit__(None, None, None)

    with jax.named_scope("s_bar"):
        pl.semaphore_wait(barrier, 5)

    class Gather:
        def __init__(self, ref, up, down, across, flow, groups, parts, srecv, precv, ssend):
            self.ref, self.up, self.down, self.across, self.flow = ref, up, down, across, flow
            self.groups, self.parts, self.srecv, self.precv, self.ssend = groups, parts, srecv, precv, ssend
            self.rows, self.here, self.sem = 0, {}, {}
            for r in sorted(groups):
                for g in groups[r]:
                    for i in g:
                        self.sem[r, i] = len(set(self.sem.values())) if i == g[0] else self.sem[r, g[0]]

        def copy(self, src, dst, size, at, rsem, dx, dy, p, other=False):
            return pltpu.make_async_remote_copy(
                src_ref=self.ref.at[src[0], src[1], pl.ds(at, size)],
                dst_ref=self.ref.at[dst[0], dst[1], pl.ds(at, size)],
                send_sem=self.ssend,
                recv_sem=rsem,
                device_id={"img": (img + images // 2) % images if other else img, "sp": dev(dx, dy, p)},
                device_id_type=MESH,
            )

        def pass_on(self, r, i, dx, dy, other=False):
            role = 4 * ((r // 4 + dy) % 2) + (r % 4 - dx) % 4
            self.copy((r, 0), (role, 0), 16, 16 * i, self.srecv.at[self.sem[role, i]], dx, dy, 0, other).start()
            self.rows += 16

        def which(self, r, which):
            return which if r in (5, 6, 7) else 0

        def slot(self, r, which):
            return 0 if self.precv is wprecv else (3 * (r - 5) + which - 1 + ROLES if which else r)

        def share(self, r, part):
            at, size, which = self.parts[part]
            which = self.which(r, which)
            self.copy((r, 0), (r, 1), size, at, self.precv.at[self.slot(r, which)], 0, 0, 1).start()
            self.rows += size

        def wait(self, r, g):
            self.copy((r, 0), (r, 0), 16 * len(g), 16 * g[0], self.srecv.at[self.sem[r, g[0]]], 0, 0, 1).wait_recv()
            assert list(g) in [list(v) for v in self.groups[r]]
            if r in (1, 3) and self.across in g:
                self.pass_on(r, self.across, 0, 1)
            here = self.here.setdefault(r, set())
            for part, (at, size, _) in enumerate(self.parts):
                mine = set(range(at // 16, (at + size) // 16))
                if mine <= here | set(g) and not mine <= here:
                    self.share(r, part)
            here.update(g)

        def wait_partner(self, r, which=0):
            size = sum(v[1] for v in self.parts if self.which(r, v[2]) == which)
            at = min(v[0] for v in self.parts if self.which(r, v[2]) == which)
            self.copy((r, 1), (r, 1), size, at, self.precv.at[self.slot(r, which)], 0, 0, 1).wait_recv()

        def own(self, lo, hi):
            for a, b in list(zip(self.up + self.down, self.down + self.up))[lo:hi]:
                self.pass_on(0, a, 1, 0)
                self.pass_on(0, b, -1, 0)

        def share_own(self):
            for part in range(len(self.parts)):
                self.share(0, part)

        def begin(self):
            self.own(0, 2)
            for n, c in enumerate(self.flow):
                self.pass_on(0, c, 0, 1)
                if n in (1, 3, 5, 7):
                    self.own(2 + n // 2, 3 + n // 2)
            self.share_own()

        def ring_all(self):
            for n, (i, j) in enumerate(zip(self.up, self.down)):
                self.ring(3, i)
                self.ring(1, j)
                if n in (1, 3):
                    self.own(6 + n // 2, 7 + n // 2)

        def ring(self, r, *g):
            self.wait(r, list(g))
            for i in g:
                self.pass_on(r, i, 1 if r == 3 else -1, 0)

        def cross(self, g):
            self.wait(4, g)
            for i in g:
                if i != self.across:
                    self.pass_on(4, i, 1, 0)
                    self.pass_on(4, i, -1, 0)

        def rest(self):
            for r, done in ((3, self.up), (1, self.down)):
                for g in self.groups[r]:
                    if g[0] not in done:
                        self.wait(r, g)

        def far(self, i):
            self.wait(2, [i])
            self.pass_on(2, i, 0, 1)

        def last(self, g):
            for r in (5, 7, 6):
                self.wait(r, g)

        def drain(self):
            total = self.ref.shape[0] * self.ref.shape[1] * self.ref.shape[2]
            assert self.rows <= total
            flat = self.ref.reshape(total, D).at[pl.ds(0, self.rows)]
            pltpu.make_async_remote_copy(
                src_ref=flat, dst_ref=flat, send_sem=self.ssend, recv_sem=self.precv.at[0],
                device_id={"sp": dev(0, 0, 1)}, device_id_type=MESH,
            ).wait_send()

    halves = [[0, 1, 2, 3], [4, 5, 6, 7]]
    pairs = [[0, 1], [2, 3], [4, 5], [6, 7]]
    groups = {
        1: [[2], [3], [6], [7], [0, 1], [4, 5]],
        2: [[i] for i in range(8)],
        3: [[0], [1], [4], [5], [2, 3], [6], [7]],
        4: halves, 5: pairs, 6: pairs, 7: pairs,
    }
    flow = [0, 2, 1, 3, 4, 6, 5, 7]
    big = ([0, 1, 4, 5], [2, 3, 6, 7], 7, flow, groups)
    row_groups = {
        1: [[2, 3], [6, 7], [0, 1], [4, 5]],
        2: [[0, 1], [2, 3], [4, 5], [6, 7]],
        3: [[0, 1], [4, 5], [2, 3], [6, 7]],
    }
    g1 = Gather(
        gat, [0, 1, 4, 5], [2, 3, 6, 7], None, None, row_groups, [(32 * j, 32, 0) for j in range(4)], nrecv, nprecv,
        ssend.at[0],
    )
    g2 = Gather(blk, *big, [(32 * j, 32, j) for j in range(4)], srecv, precv, ssend.at[1])
    whole = [[0, 1, 2, 3, 4]]
    two = [[0, 1, 2], [3, 4]]
    wgroups = {
        1: [[4], [3], [2], [0, 1]],
        2: [[i] for i in range(5)],
        3: [[0], [1], [2], [3, 4]],
        4: whole, 5: two, 6: two, 7: two,
    }
    gw = Gather(wg, [0, 1, 2], [4, 3], None, None, wgroups, [(0, 48, 0), (48, 32, 0)], wsrecv, wprecv, ssend.at[2])

    def w_near(r, g):
        gw.wait(r, g)
        for i in g:
            if i in (gw.up if r == 3 else gw.down):
                gw.pass_on(r, i, 1 if r == 3 else -1, 0)
        for i in g:
            if r == 3 and i != 4:
                gw.pass_on(r, i, 0, 1, True)

    def w_cross():
        gw.wait(4, whole[0])
        gw.pass_on(4, 4, 1, 0)
        for i in (4, 3, 2, 1, 0):
            gw.pass_on(4, i, -1, 0)

    def w_far(i):
        gw.wait(2, [i])
        gw.pass_on(2, i, 0, 1, True)

    def head_weights(at, size, sem, other=False):
        return pltpu.make_async_remote_copy(
            src_ref=wqv.at[pl.ds(at, size)], dst_ref=wqo.at[pl.ds(at, size)], send_sem=hsend.at[0], recv_sem=hrecv.at[sem],
            device_id={"img": (img + images // 2) % images if other else img, "sp": dev(0, 1, 0)}, device_id_type=MESH,
        )

    g1.own(0, 8)
    loads[3].wait()
    for i in range(15):
        head_weights(16 * i, 16, 0 if i < 10 else 1, i % 2 == 0).start()
    loads[4].wait()
    for i in range(5):
        gw.pass_on(0, i, 0, 1, True)
    g1.share_own()
    gw.share_own()

    for load in loads[5:8]:
        load.wait()
    lane = lax.broadcasted_iota(jnp.int32, (HDIM, D), 1)
    sub = lax.broadcasted_iota(jnp.int32, (HDIM, D), 0)
    for n, head in enumerate((me, dev(0, 1, 0))):
        mine = lane == sub + head * HDIM
        for c in range(3):
            col = jnp.sum(jnp.where(mine, bq_ref[c : c + 1, :], 0.0), axis=1, keepdims=True)
            bcol[3 * n + c] = jnp.broadcast_to(col, (HDIM, 128))
    same = lax.broadcasted_iota(jnp.int32, (SHARE, SHARE), 0) == lax.broadcasted_iota(
        jnp.int32, (SHARE, SHARE), 1
    )
    col = jnp.sum(jnp.where(same, fb_ref[...].reshape(1, SHARE), 0.0), axis=1, keepdims=True)
    fcol[...] = jnp.broadcast_to(col, (SHARE, 128))
    for r in range(4):
        at = [pl.multiple_of(dev(r, 0, p) * 128, 128) for p in range(2)]
        prow = jnp.concatenate([pos_ref[0:1, pl.ds(a, 128)] for a in at], axis=1).astype(jnp.float32)
        pcol = jnp.concatenate([pos_ref[1:2, pl.ds(a, 128)] for a in at], axis=1).astype(jnp.float32)
        row = lax.broadcasted_iota(jnp.int32, (40, 256), 0)
        power = jnp.where(row < 20, row, row - 20).astype(jnp.float32)
        inv = jnp.exp2(power * (-math.log2(10000.0) / 20.0))
        angle = jnp.where(row < 20, prow, pcol) * inv
        trig[r, 0] = jnp.cos(angle)
        trig[r, 1] = jnp.sin(angle)
    for r in range(4, ROLES):
        qt[r, HDIM:128] = jnp.zeros((128 - HDIM, 256), jnp.bfloat16)

    def project(weights, r, ps):
        rows = gat[r, ps[0] : ps[-1] + 1].reshape(128 * len(ps), D)
        return lax.dot_general(weights, rows, (((1,), (1,)), ((), ())), preferred_element_type=jnp.float32)

    def finish_head(v, r, ps, n, c):
        v = v + jnp.concatenate([bcol[3 * n + c]] * len(ps), axis=1)
        if c == 2:
            return v
        cos, sin = (trig[r, t, :, pl.ds(128 * ps[0], 128 * len(ps))] for t in range(2))
        lo, hi = v[:40], v[40:]
        return jnp.concatenate([lo * cos - hi * sin, hi * cos + lo * sin], axis=0)

    def turned_keys(k):
        return jnp.concatenate([k, jnp.zeros((128 - HDIM, 256), jnp.float32)], axis=0).T.astype(jnp.bfloat16)

    def qkv(r):
        out = project(wqv[...], r, (0, 1))
        q, k, v = (finish_head(out[80 * c : 80 * c + 80], r, (0, 1), 0, c) for c in range(3))
        qt[r] = jnp.concatenate([q, jnp.zeros((128 - HDIM, 256), jnp.float32)], axis=0).astype(jnp.bfloat16)
        kk[r] = turned_keys(k)
        vt[r] = v.astype(jnp.bfloat16)

    def qkv_other(r, ps, cs=(0, 1, 2)):
        out = project(wqo[80 * cs[0] : 80 * cs[-1] + 80], r, ps)
        lanes = pl.ds(128 * ps[0], 128 * len(ps))
        for n, c in enumerate(cs):
            stage[r, c, :, lanes] = finish_head(out[80 * n : 80 * n + 80], r, ps, 1, c).astype(jnp.bfloat16)
        for c in cs:
            dst = (qt.at[4 + r, pl.ds(0, HDIM), lanes], kin.at[r, :, lanes], vt.at[4 + r, :, lanes])[c]
            pltpu.make_async_remote_copy(
                src_ref=stage.at[r, c, :, lanes], dst_ref=dst, send_sem=hsend.at[1], recv_sem=hrecv.at[2 + r],
                device_id={"img": img, "sp": dev(0, 1, 0)}, device_id_type=MESH,
            ).start()

    def receive(r):
        pltpu.make_async_remote_copy(
            src_ref=stage.at[r], dst_ref=stage.at[r], send_sem=hsend.at[1], recv_sem=hrecv.at[2 + r],
            device_id={"img": img, "sp": dev(0, 1, 0)}, device_id_type=MESH,
        ).wait_recv()
        kk[4 + r] = turned_keys(kin[r].astype(jnp.float32))

    early, late = (0, 3, 1, 2, 4), (7, 5, 6)

    def score(r, slot, keys):
        top = None
        for n, c in enumerate(keys):
            s = jnp.dot(kk[c], qt[r], preferred_element_type=jnp.float32)
            sc[slot, n] = s
            m = jnp.max(s.reshape(32, 8, 256), axis=0)
            top = m if top is None else jnp.maximum(top, m)
        return jnp.max(top, axis=0, keepdims=True) * SCALE

    def weigh(slot, keys, top):
        total, out = None, None
        for n, c in enumerate(keys):
            w = jnp.exp2(sc[slot, n] * SCALE - top)
            s = jnp.sum(w.reshape(32, 8, 256), axis=0)
            o = jnp.dot(vt[c], w.astype(jnp.bfloat16), preferred_element_type=jnp.float32)
            total = s if total is None else total + s
            out = o if out is None else out + o
        return jnp.sum(total, axis=0, keepdims=True), out

    def begin_tile(n, top):
        later = score(early[n + 1], (n + 1) % 2, early) if n < 4 else None
        total, out = weigh(n % 2, early, top)
        osum[n] = out
        stat[n, 0:1] = top
        stat[n, 1:2] = total
        return later

    def end_tile(r, slot, top):
        if r in early:
            n = early.index(r)
            before = stat[n, 0:1]
            both = jnp.maximum(before, top)
            total, out = weigh(slot, late, both)
            old = jnp.exp2(before - both)
            total, out = total + stat[n, 1:2] * old, out + osum[n] * old
        else:
            total, out = weigh(slot, early + late, top)
        out = (out / total).astype(jnp.bfloat16)
        for p in range(2):
            osend[2 * r + p] = out[:, p * 128 : (p + 1) * 128]

    with jax.named_scope("a_own"):
        g1.wait_partner(0)
        qkv(0)
    with jax.named_scope("a_ring"):
        g1.ring(3, 0, 1)
        g1.ring(1, 2, 3)
        g1.ring(3, 4, 5)
        g1.ring(1, 6, 7)
        gw.own(0, 5)
    with jax.named_scope("a_other0"):
        head_weights(0, 160, 0).wait_recv()
        qkv_other(0, (0, 1), (0, 1))
    with jax.named_scope("a_rest"):
        for r in (3, 1):
            g1.wait(r, row_groups[r][2])
            g1.wait(r, row_groups[r][3])
    with jax.named_scope("a_other0v"):
        head_weights(160, 80, 1).wait_recv()
        qkv_other(0, (0, 1), (2,))
    with jax.named_scope("a_near"):
        for r in (3, 1):
            qkv_other(r, (0,))
    with jax.named_scope("a_near_p"):
        for r in (3, 1):
            g1.wait_partner(r)
            qkv_other(r, (1,))
    with jax.named_scope("a_near_own"):
        qkv(3)
        qkv(1)
    with jax.named_scope("a_two"):
        for g in row_groups[2]:
            g1.wait(2, g)
        qkv_other(2, (0,))
    with jax.named_scope("w_ring0"):
        w_near(3, [0])
        w_near(1, [4])
    with jax.named_scope("a_two_p"):
        g1.wait_partner(2)
        qkv_other(2, (1,))
        qkv(2)
    with jax.named_scope("w_ring1"):
        w_near(3, [1])
        w_near(1, [3])
    with jax.named_scope("a_recv0"):
        receive(0)
    with jax.named_scope("a_early0"):
        top = score(early[0], 0, early)
        top = begin_tile(0, top)
    with jax.named_scope("w_ring2"):
        w_near(3, [2])
        w_near(1, [2])
        w_cross()
    with jax.named_scope("a_early1"):
        top = begin_tile(1, top)
    with jax.named_scope("w_ring3"):
        w_near(3, [3, 4])
        w_near(1, [0, 1])
    with jax.named_scope("a_recv3"):
        receive(3)
    with jax.named_scope("a_early2"):
        top = begin_tile(2, top)
        top = begin_tile(3, top)
    with jax.named_scope("w_far0"):
        w_far(0)
        w_far(4)
    with jax.named_scope("a_recv1"):
        receive(1)
    with jax.named_scope("a_early3"):
        begin_tile(4, top)
    with jax.named_scope("w_far1"):
        w_far(1)
        w_far(3)
    with jax.named_scope("a_recv2"):
        receive(2)

    def give(r):
        for p in range(2):
            if r == 0 and p == 0:
                continue
            role = 4 * (r // 4) + (-r % 4) % 4
            pltpu.make_async_remote_copy(
                src_ref=osend.at[2 * r + p],
                dst_ref=att.at[2 * role + p],
                send_sem=asem.at[0],
                recv_sem=asem.at[1],
                device_id={"sp": dev(r % 4, r // 4, p)},
                device_id_type=MESH,
            ).start()

    order = (6, 7, 5, 2, 4, 3, 1, 0)
    def keys(r):
        return late if r in early else early + late

    top = score(order[0], 0, keys(order[0]))
    for i, r in enumerate(order):
        if i + 1 < ROLES:
            later = score(order[i + 1], (i + 1) % 2, keys(order[i + 1]))
        end_tile(r, i % 2, top)
        top = later
        if i > 0:
            give(order[i - 1])
        if i == 0:
            with jax.named_scope("w_far2"):
                w_far(2)
    with jax.named_scope("t_give"):
        give(order[-1])
        att[0] = osend[0]
    with jax.named_scope("w_last"):
        gw.last(two[0])
        gw.last(two[1])
    with jax.named_scope("w_partner"):
        pltpu.make_async_remote_copy(
            src_ref=wg.at[:, 1], dst_ref=wg.at[:, 1], send_sem=ssend.at[2], recv_sem=wprecv.at[0],
            device_id={"img": img, "sp": dev(0, 0, 1)}, device_id_type=MESH,
        ).wait_recv()
    with jax.named_scope("t_back"):
        pltpu.make_async_remote_copy(
            src_ref=osend.at[pl.ds(1, 15)], dst_ref=att.at[pl.ds(1, 15)], send_sem=asem.at[0], recv_sem=asem.at[1],
            device_id={"sp": dev(0, 0, 1)}, device_id_type=MESH,
        ).wait_recv()

    for load in loads[8:11]:
        load.wait()
    got = att[...].reshape(D, 128).T
    out = jnp.dot(got, wg[...].reshape(D, D), preferred_element_type=jnp.float32)
    vit = (x_ref[...].astype(jnp.float32) + out + pb_ref[...].reshape(1, D)).astype(jnp.bfloat16)
    vit_ref[...] = vit
    zn = norm_rows(vit.astype(jnp.float32), g2_ref[...].reshape(1, D), b2_ref[...].reshape(1, D))
    for b in range(D // 128):
        zf[b] = zn[:, b * 128 : (b + 1) * 128]
    for j in range(4):
        for b in range(D // 128):
            blk[0, 0, pl.ds(j * 32, 32), pl.ds(b * 128, 128)] = zf[
                b, pl.ds(j, 32, stride=4), :
            ].astype(jnp.bfloat16)

    g2.begin()
    loads[11].wait()

    def fc1(dy, j):
        parts = []
        for ax in range(4):
            r = 4 * dy + (ax + 4 - mx) % 4
            for c in range(2):
                parts.append(blk[r, (c + core) % 2, pl.ds(j * 32, 32)])
        return lax.dot_general(
            fcv[:, j * D : (j + 1) * D],
            jnp.concatenate(parts, axis=0),
            (((1,), (1,)), ((), ())),
            preferred_element_type=jnp.float32,
        )

    def finish(dy, total):
        v = total + jnp.concatenate([fcol[...], fcol[...]], axis=1)
        at = pl.multiple_of(((my + dy) % 2) * 256, 256)
        hid_ref[:, pl.ds(at, 256)] = (0.5 * v * (1.0 + lax.erf(v * (2.0**-0.5)))).astype(jnp.bfloat16)

    with jax.named_scope("b_ring"):
        g2.ring_all()
    with jax.named_scope("b_cross"):
        g2.cross(halves[0])
    with jax.named_scope("b_far0"):
        for i in flow[:4]:
            g2.far(i)
    with jax.named_scope("b_cross1"):
        g2.cross(halves[1])
    with jax.named_scope("b_far1"):
        for i in flow[4:]:
            g2.far(i)
    with jax.named_scope("b_rest"):
        g2.rest()
    def partner(j):
        with jax.named_scope(f"b_partner{j}"):
            for r in (5, 7, 6):
                g2.wait_partner(r, j)

    with jax.named_scope("b_last0"):
        g2.last(pairs[0])
    with jax.named_scope("b_far_p"):
        for r in (0, 3, 1, 2, 4):
            g2.wait_partner(r)
    with jax.named_scope("b_fc1_a"):
        acc[...] = fc1(0, 0) + fc1(0, 1)
    with jax.named_scope("b_last1"):
        g2.last(pairs[1])
    with jax.named_scope("b_fc1_b"):
        finish(0, acc[...] + fc1(0, 2) + fc1(0, 3))
    partner(0)
    with jax.named_scope("b_fc1_c"):
        acc[...] = fc1(1, 0)
    partner(1)
    with jax.named_scope("b_fc1_d"):
        acc[...] += fc1(1, 1)
    with jax.named_scope("b_last2"):
        g2.last(pairs[2])
    with jax.named_scope("b_last3"):
        g2.last(pairs[3])
    partner(2)
    with jax.named_scope("b_fc1_e"):
        acc[...] += fc1(1, 2)
    partner(3)
    with jax.named_scope("b_fc1_f"):
        finish(1, acc[...] + fc1(1, 3))

    with jax.named_scope("drain"):
        for g in (g1, gw, g2):
            g.drain()
        head_weights(0, 3 * HDIM, 0).wait_send()
        pltpu.make_async_remote_copy(
            src_ref=stage, dst_ref=stage, send_sem=hsend.at[1], recv_sem=hrecv.at[2],
            device_id={"img": img, "sp": dev(0, 1, 0)}, device_id_type=MESH,
        ).wait_send()
        pltpu.make_async_remote_copy(
            src_ref=osend.at[pl.ds(1, 15)], dst_ref=att.at[pl.ds(1, 15)], send_sem=asem.at[0], recv_sem=asem.at[1],
            device_id={"sp": dev(0, 0, 1)}, device_id_type=MESH,
        ).wait_send()


def put(vit_ref, hid_ref, vit_hbm, hid_hbm, sem):
    copies = [
        pltpu.make_async_copy(vit_ref, vit_hbm, sem.at[0]),
        pltpu.make_async_copy(hid_ref, hid_hbm, sem.at[1]),
    ]
    for copy in copies:
        copy.start()
    for copy in copies:
        copy.wait()


def per_device(
    patches, pos_ids, norm_gain, norm_bias, qkv_weight, qkv_bias, proj_weight, proj_bias, merge_gain, merge_bias,
    fc1_weight, fc1_bias,
):
    vmem = pl.BlockSpec(memory_space=pltpu.VMEM)
    hbm = pl.BlockSpec(memory_space=pl.ANY)
    bf, f32 = jnp.bfloat16, jnp.float32
    dma = pltpu.SemaphoreType.DMA
    vit, hid = pl.pallas_call(
        kernel,
        out_shape=(pltpu.VMEM((128, D), bf), pltpu.VMEM((SHARE, 512), bf)),
        in_specs=[hbm] * 12,
        out_specs=(vmem, vmem),
        scratch_shapes=[
            pltpu.VMEM((128, D), bf),
            pltpu.VMEM((2, PATCHES), jnp.int32),
            pltpu.VMEM((D,), f32),
            pltpu.VMEM((D,), f32),
            pltpu.VMEM((3, D), f32),
            pltpu.VMEM((D,), f32),
            pltpu.VMEM((D,), f32),
            pltpu.VMEM((D,), f32),
            pltpu.VMEM((SHARE,), f32),
            pltpu.VMEM((4, 2, 128, D), bf),
            pltpu.VMEM((ROLES, 2, 128, D), bf),
            pltpu.VMEM((ROLES, 2, HDIM, D), bf),
            pltpu.VMEM((2 * ROLES, HDIM, 128), bf),
            pltpu.VMEM((2 * ROLES, HDIM, 128), bf),
            pltpu.VMEM((ROLES, 128, 256), bf),
            pltpu.VMEM((ROLES, 256, 128), bf),
            pltpu.VMEM((ROLES, HDIM, 256), bf),
            pltpu.VMEM((2, ROLES, 256, 256), f32),
            pltpu.VMEM((SHARE, HIDDEN), bf),
            pltpu.VMEM((3 * HDIM, D), bf),
            pltpu.VMEM((6, HDIM, 128), f32),
            pltpu.VMEM((SHARE, 128), f32),
            pltpu.VMEM((D // 128, 128, 128), f32),
            pltpu.VMEM((SHARE, 256), f32),
            pltpu.VMEM((5, HDIM, 256), f32),
            pltpu.VMEM((5, 8, 256), f32),
            pltpu.VMEM((3 * HDIM, D), bf),
            pltpu.VMEM((4, 2, 40, 256), f32),
            pltpu.VMEM((4, 3, HDIM, 256), bf),
            pltpu.VMEM((4, HDIM, 256), bf),
            dma((3,)),
            dma((12,)),
            dma((4,)),
            dma((35,)),
            dma((ROLES + 9,)),
            dma((20,)),
            dma((1,)),
            dma((2,)),
            dma((6,)),
            dma((2,)),
            dma((12,)),
        ],
        compiler_params=pltpu.CompilerParams(
            collective_id=0, has_side_effects=True, vmem_limit_bytes=58 * 1024 * 1024
        ),
    )(
        patches,
        pos_ids,
        norm_gain,
        norm_bias,
        qkv_weight.transpose(1, 2, 0).reshape(3 * HDIM, D),
        qkv_bias,
        proj_weight,
        proj_bias,
        merge_gain,
        merge_bias,
        fc1_weight.T,
        fc1_bias,
    )
    vit, hid = pl.pallas_call(
        put,
        out_shape=(jax.ShapeDtypeStruct((128, D), bf), jax.ShapeDtypeStruct((SHARE, 512), bf)),
        in_specs=[vmem, vmem],
        out_specs=(hbm, hbm),
        scratch_shapes=[dma((2,))],
    )(pltpu.with_memory_space_constraint(vit, pltpu.VMEM), pltpu.with_memory_space_constraint(hid, pltpu.VMEM))
    return vit, hid.T


def solution(mesh):
    return jax.shard_map(
        per_device,
        mesh=mesh,
        in_specs=(
            P(("img", "sp"), None),
            P(None, "img"),
            P(),
            P(),
            P(None, None, "sp"),
            P(),
            P("sp", None),
            P(),
            P(),
            P(),
            P(None, "sp"),
            P("sp"),
        ),
        out_specs=(P(("img", "sp"), None), P("img", "sp")),
        check_vma=False,
    )
```

```python
import math

import jax
import jax.numpy as jnp
from jax import lax
from jax.experimental import pallas as pl
from jax.experimental.pallas import tpu as pltpu
from jax.sharding import PartitionSpec as P

MESH = pl.DeviceIdType.MESH
HEADS = 16
D = 1280
HDIM = 80
PATCHES = 2048
HIDDEN = 5120
SHARE = 320
ROLES = 8
SCALE = math.log2(math.e) / math.sqrt(HDIM)


def norm_rows(v, gain, bias):
    mean = jnp.mean(v, axis=-1, keepdims=True)
    cen = v - mean
    var = jnp.mean(cen * cen, axis=-1, keepdims=True)
    return cen * lax.rsqrt(var + 1e-06) * gain + bias


def kernel(
    x_hbm, pos_hbm, g1_hbm, b1_hbm, wq_hbm, bq_hbm, wp_hbm, pb_hbm, g2_hbm, b2_hbm, fc_hbm, fb_hbm,
    vit_ref, hid_ref, x_ref, pos_ref, g1_ref, b1_ref, bq_ref, pb_ref, g2_ref, b2_ref, fb_ref,
    gat, blk, wg, att, osend, qt, kk, vt, sc, fcv, wqv, bcol, fcol, zf, acc, osum, stat,
    wqo, trig, stage, kin, ssend, srecv, precv, wsrecv, wprecv, hsend, hrecv, asem, local,
):
    me = lax.axis_index("sp")
    img, images = lax.axis_index("img"), lax.axis_size("img")
    core = me % 2
    mx = (me // 2) % 4
    my = me // 8

    def dev(dx, dy, p):
        return ((my + dy) % 2) * 8 + ((mx + dx) % 4) * 2 + (core + p) % 2

    barrier = pltpu.get_barrier_semaphore()
    for near in (dev(1, 0, 0), dev(-1, 0, 0), dev(0, 1, 0), dev(0, 0, 1)):
        pl.semaphore_signal(barrier, inc=1, device_id={"img": img, "sp": near}, device_id_type=MESH)
    pl.semaphore_signal(barrier, inc=1, device_id={"img": (img + images // 2) % images, "sp": dev(0, 1, 0)}, device_id_type=MESH)

    loads = [
        (x_hbm, x_ref), (g1_hbm, g1_ref), (b1_hbm, b1_ref), (wq_hbm, wqv), (wp_hbm, wg.at[0, 0]), (bq_hbm, bq_ref),
        (fb_hbm, fb_ref), (pos_hbm, pos_ref), (pb_hbm, pb_ref), (g2_hbm, g2_ref), (b2_hbm, b2_ref), (fc_hbm, fcv),
    ]
    loads = [pltpu.make_async_copy(src, dst, local.at[i]) for i, (src, dst) in enumerate(loads)]
    for load in loads:
        load.start()
    with jax.named_scope("s_load"):
        for load in loads[:3]:
            load.wait()

    ln_scope = jax.named_scope("s_ln")
    ln_scope.__enter__()
    xf = x_ref[...].astype(jnp.float32)
    normed = norm_rows(xf, g1_ref[...].reshape(1, D), b1_ref[...].reshape(1, D)).astype(jnp.bfloat16)
    gat[0, 0] = normed
    ln_scope.__exit__(None, None, None)

    with jax.named_scope("s_bar"):
        pl.semaphore_wait(barrier, 5)

    class Gather:
        def __init__(self, ref, up, down, across, flow, groups, parts, srecv, precv, ssend):
            self.ref, self.up, self.down, self.across, self.flow = ref, up, down, across, flow
            self.groups, self.parts, self.srecv, self.precv, self.ssend = groups, parts, srecv, precv, ssend
            self.rows, self.here, self.sem = 0, {}, {}
            for r in sorted(groups):
                for g in groups[r]:
                    for i in g:
                        self.sem[r, i] = len(set(self.sem.values())) if i == g[0] else self.sem[r, g[0]]

        def copy(self, src, dst, size, at, rsem, dx, dy, p, other=False):
            return pltpu.make_async_remote_copy(
                src_ref=self.ref.at[src[0], src[1], pl.ds(at, size)],
                dst_ref=self.ref.at[dst[0], dst[1], pl.ds(at, size)],
                send_sem=self.ssend,
                recv_sem=rsem,
                device_id={"img": (img + images // 2) % images if other else img, "sp": dev(dx, dy, p)},
                device_id_type=MESH,
            )

        def pass_on(self, r, i, dx, dy, other=False):
            role = 4 * ((r // 4 + dy) % 2) + (r % 4 - dx) % 4
            self.copy((r, 0), (role, 0), 16, 16 * i, self.srecv.at[self.sem[role, i]], dx, dy, 0, other).start()
            self.rows += 16

        def which(self, r, which):
            return which if r in (5, 6, 7) else 0

        def slot(self, r, which):
            return 0 if self.precv is wprecv else (3 * (r - 5) + which - 1 + ROLES if which else r)

        def share(self, r, part):
            at, size, which = self.parts[part]
            which = self.which(r, which)
            self.copy((r, 0), (r, 1), size, at, self.precv.at[self.slot(r, which)], 0, 0, 1).start()
            self.rows += size

        def wait(self, r, g):
            self.copy((r, 0), (r, 0), 16 * len(g), 16 * g[0], self.srecv.at[self.sem[r, g[0]]], 0, 0, 1).wait_recv()
            assert list(g) in [list(v) for v in self.groups[r]]
            if r in (1, 3) and self.across in g:
                self.pass_on(r, self.across, 0, 1)
            here = self.here.setdefault(r, set())
            for part, (at, size, _) in enumerate(self.parts):
                mine = set(range(at // 16, (at + size) // 16))
                if mine <= here | set(g) and not mine <= here:
                    self.share(r, part)
            here.update(g)

        def wait_partner(self, r, which=0):
            size = sum(v[1] for v in self.parts if self.which(r, v[2]) == which)
            at = min(v[0] for v in self.parts if self.which(r, v[2]) == which)
            self.copy((r, 1), (r, 1), size, at, self.precv.at[self.slot(r, which)], 0, 0, 1).wait_recv()

        def own(self, lo, hi):
            for a, b in list(zip(self.up + self.down, self.down + self.up))[lo:hi]:
                self.pass_on(0, a, 1, 0)
                self.pass_on(0, b, -1, 0)

        def share_own(self):
            for part in range(len(self.parts)):
                self.share(0, part)

        def begin(self):
            self.own(0, 2)
            for n, c in enumerate(self.flow):
                self.pass_on(0, c, 0, 1)
                if n in (1, 3, 5, 7):
                    self.own(2 + n // 2, 3 + n // 2)
            self.share_own()

        def ring_all(self):
            for n, (i, j) in enumerate(zip(self.up, self.down)):
                self.ring(3, i)
                self.ring(1, j)
                if n in (1, 3):
                    self.own(6 + n // 2, 7 + n // 2)

        def ring(self, r, *g):
            self.wait(r, list(g))
            for i in g:
                self.pass_on(r, i, 1 if r == 3 else -1, 0)

        def cross(self, g):
            self.wait(4, g)
            for i in g:
                if i != self.across:
                    self.pass_on(4, i, 1, 0)
                    self.pass_on(4, i, -1, 0)

        def rest(self):
            for r, done in ((3, self.up), (1, self.down)):
                for g in self.groups[r]:
                    if g[0] not in done:
                        self.wait(r, g)

        def far(self, i):
            self.wait(2, [i])
            self.pass_on(2, i, 0, 1)

        def last(self, g):
            for r in (5, 7, 6):
                self.wait(r, g)

        def drain(self):
            total = self.ref.shape[0] * self.ref.shape[1] * self.ref.shape[2]
            assert self.rows <= total
            flat = self.ref.reshape(total, D).at[pl.ds(0, self.rows)]
            pltpu.make_async_remote_copy(
                src_ref=flat, dst_ref=flat, send_sem=self.ssend, recv_sem=self.precv.at[0],
                device_id={"sp": dev(0, 0, 1)}, device_id_type=MESH,
            ).wait_send()

    halves = [[0, 1, 2, 3], [4, 5, 6, 7]]
    pairs = [[0, 1], [2, 3], [4, 5], [6, 7]]
    groups = {
        1: [[2], [3], [6], [7], [0, 1], [4, 5]],
        2: [[i] for i in range(8)],
        3: [[0], [1], [4], [5], [2, 3], [6], [7]],
        4: halves, 5: pairs, 6: pairs, 7: pairs,
    }
    flow = [0, 2, 1, 3, 4, 6, 5, 7]
    big = ([0, 1, 4, 5], [2, 3, 6, 7], 7, flow, groups)
    row_groups = {
        1: [[2, 3], [6, 7], [0, 1], [4, 5]],
        2: [[0, 1], [2, 3], [4, 5], [6, 7]],
        3: [[0, 1], [4, 5], [2, 3], [6, 7]],
    }
    g1 = Gather(
        gat, [0, 1, 4, 5], [2, 3, 6, 7], None, None, row_groups, [(32 * j, 32, 0) for j in range(4)], srecv, precv,
        ssend.at[0],
    )
    g2 = Gather(blk, *big, [(32 * j, 32, j) for j in range(4)], srecv, precv, ssend.at[1])
    whole = [[0, 1, 2, 3, 4]]
    two = [[0, 1, 2], [3, 4]]
    wgroups = {
        1: [[4], [3], [2], [0, 1]],
        2: [[i] for i in range(5)],
        3: [[0], [1], [2], [3, 4]],
        4: whole, 5: two, 6: two, 7: two,
    }
    gw = Gather(wg, [0, 1, 2], [4, 3], None, None, wgroups, [(0, 48, 0), (48, 32, 0)], wsrecv, wprecv, ssend.at[2])

    def w_near(r, g):
        gw.wait(r, g)
        for i in g:
            if i in (gw.up if r == 3 else gw.down):
                gw.pass_on(r, i, 1 if r == 3 else -1, 0)
        for i in g:
            if r == 3 and i != 4:
                gw.pass_on(r, i, 0, 1, True)

    def w_cross():
        gw.wait(4, whole[0])
        gw.pass_on(4, 4, 1, 0)
        for i in range(5):
            gw.pass_on(4, i, -1, 0)

    def w_far(i):
        gw.wait(2, [i])
        gw.pass_on(2, i, 0, 1, True)

    def head_weights(at, size, sem, other=False):
        return pltpu.make_async_remote_copy(
            src_ref=wqv.at[pl.ds(at, size)], dst_ref=wqo.at[pl.ds(at, size)], send_sem=hsend.at[0], recv_sem=hrecv.at[sem],
            device_id={"img": (img + images // 2) % images if other else img, "sp": dev(0, 1, 0)}, device_id_type=MESH,
        )

    g1.own(0, 8)
    loads[3].wait()
    for i in range(15):
        head_weights(16 * i, 16, 0 if i < 10 else 1, i % 2 == 0).start()
    loads[4].wait()
    for i in range(5):
        gw.pass_on(0, i, 0, 1, True)
    g1.share_own()
    gw.share_own()

    for load in loads[5:8]:
        load.wait()
    lane = lax.broadcasted_iota(jnp.int32, (HDIM, D), 1)
    sub = lax.broadcasted_iota(jnp.int32, (HDIM, D), 0)
    for n, head in enumerate((me, dev(0, 1, 0))):
        mine = lane == sub + head * HDIM
        for c in range(3):
            col = jnp.sum(jnp.where(mine, bq_ref[c : c + 1, :], 0.0), axis=1, keepdims=True)
            bcol[3 * n + c] = jnp.broadcast_to(col, (HDIM, 128))
    same = lax.broadcasted_iota(jnp.int32, (SHARE, SHARE), 0) == lax.broadcasted_iota(
        jnp.int32, (SHARE, SHARE), 1
    )
    col = jnp.sum(jnp.where(same, fb_ref[...].reshape(1, SHARE), 0.0), axis=1, keepdims=True)
    fcol[...] = jnp.broadcast_to(col, (SHARE, 128))
    for r in range(4):
        at = [pl.multiple_of(dev(r, 0, p) * 128, 128) for p in range(2)]
        prow = jnp.concatenate([pos_ref[0:1, pl.ds(a, 128)] for a in at], axis=1).astype(jnp.float32)
        pcol = jnp.concatenate([pos_ref[1:2, pl.ds(a, 128)] for a in at], axis=1).astype(jnp.float32)
        row = lax.broadcasted_iota(jnp.int32, (40, 256), 0)
        power = jnp.where(row < 20, row, row - 20).astype(jnp.float32)
        inv = jnp.exp2(power * (-math.log2(10000.0) / 20.0))
        angle = jnp.where(row < 20, prow, pcol) * inv
        trig[r, 0] = jnp.cos(angle)
        trig[r, 1] = jnp.sin(angle)
    for r in range(4, ROLES):
        qt[r, HDIM:128] = jnp.zeros((128 - HDIM, 256), jnp.bfloat16)

    def project(weights, r, ps):
        rows = gat[r, ps[0] : ps[-1] + 1].reshape(128 * len(ps), D)
        return lax.dot_general(weights, rows, (((1,), (1,)), ((), ())), preferred_element_type=jnp.float32)

    def finish_head(v, r, ps, n, c):
        v = v + jnp.concatenate([bcol[3 * n + c]] * len(ps), axis=1)
        if c == 2:
            return v
        cos, sin = (trig[r, t, :, pl.ds(128 * ps[0], 128 * len(ps))] for t in range(2))
        lo, hi = v[:40], v[40:]
        return jnp.concatenate([lo * cos - hi * sin, hi * cos + lo * sin], axis=0)

    def turned_keys(k):
        return jnp.concatenate([k, jnp.zeros((128 - HDIM, 256), jnp.float32)], axis=0).T.astype(jnp.bfloat16)

    def qkv(r):
        out = project(wqv[...], r, (0, 1))
        q, k, v = (finish_head(out[80 * c : 80 * c + 80], r, (0, 1), 0, c) for c in range(3))
        qt[r] = jnp.concatenate([q, jnp.zeros((128 - HDIM, 256), jnp.float32)], axis=0).astype(jnp.bfloat16)
        kk[r] = turned_keys(k)
        vt[r] = v.astype(jnp.bfloat16)

    def qkv_other(r, ps, cs=(0, 1, 2)):
        out = project(wqo[80 * cs[0] : 80 * cs[-1] + 80], r, ps)
        lanes = pl.ds(128 * ps[0], 128 * len(ps))
        for n, c in enumerate(cs):
            stage[r, c, :, lanes] = finish_head(out[80 * n : 80 * n + 80], r, ps, 1, c).astype(jnp.bfloat16)
        for c in cs:
            dst = (qt.at[4 + r, pl.ds(0, HDIM), lanes], kin.at[r, :, lanes], vt.at[4 + r, :, lanes])[c]
            pltpu.make_async_remote_copy(
                src_ref=stage.at[r, c, :, lanes], dst_ref=dst, send_sem=hsend.at[1], recv_sem=hrecv.at[2 + r],
                device_id={"img": img, "sp": dev(0, 1, 0)}, device_id_type=MESH,
            ).start()

    def receive(r):
        pltpu.make_async_remote_copy(
            src_ref=stage.at[r], dst_ref=stage.at[r], send_sem=hsend.at[1], recv_sem=hrecv.at[2 + r],
            device_id={"img": img, "sp": dev(0, 1, 0)}, device_id_type=MESH,
        ).wait_recv()
        kk[4 + r] = turned_keys(kin[r].astype(jnp.float32))

    early, late, ahead = (0, 3, 1, 2, 4), (7, 5, 6), (0, 3, 1, 2, 4, 7, 5)

    def score(r, slot, keys):
        top = None
        for n, c in enumerate(keys):
            s = jnp.dot(kk[c], qt[r], preferred_element_type=jnp.float32)
            sc[slot, n] = s
            m = jnp.max(s.reshape(32, 8, 256), axis=0)
            top = m if top is None else jnp.maximum(top, m)
        return jnp.max(top, axis=0, keepdims=True) * SCALE

    def weigh(slot, keys, top):
        total, out = None, None
        for n, c in enumerate(keys):
            w = jnp.exp2(sc[slot, n] * SCALE - top)
            s = jnp.sum(w.reshape(32, 8, 256), axis=0)
            o = jnp.dot(vt[c], w.astype(jnp.bfloat16), preferred_element_type=jnp.float32)
            total = s if total is None else total + s
            out = o if out is None else out + o
        return jnp.sum(total, axis=0, keepdims=True), out

    def begin_tile(n, top, more=True):
        later = score(ahead[n + 1], (n + 1) % 2, early) if more else None
        total, out = weigh(n % 2, early, top)
        osum[n] = out
        stat[n, 0:1] = top
        stat[n, 1:2] = total
        return later

    def end_tile(r, slot, top):
        if r in ahead:
            n = ahead.index(r)
            before = stat[n, 0:1]
            both = jnp.maximum(before, top)
            total, out = weigh(slot, late, both)
            old = jnp.exp2(before - both)
            total, out = total + stat[n, 1:2] * old, out + osum[n] * old
        else:
            total, out = weigh(slot, early + late, top)
        out = (out / total).astype(jnp.bfloat16)
        for p in range(2):
            osend[2 * r + p] = out[:, p * 128 : (p + 1) * 128]

    with jax.named_scope("a_own"):
        g1.wait_partner(0)
        qkv(0)
    with jax.named_scope("a_ring"):
        g1.ring(3, 0, 1)
        g1.ring(1, 2, 3)
        g1.ring(3, 4, 5)
        g1.ring(1, 6, 7)
        gw.own(0, 5)
    with jax.named_scope("a_other0"):
        head_weights(0, 160, 0).wait_recv()
        qkv_other(0, (0, 1), (0, 1))
    with jax.named_scope("a_rest"):
        for r in (3, 1):
            g1.wait(r, row_groups[r][2])
            g1.wait(r, row_groups[r][3])
    with jax.named_scope("a_other0v"):
        head_weights(160, 80, 1).wait_recv()
        qkv_other(0, (0, 1), (2,))
    with jax.named_scope("a_near"):
        for r in (3, 1):
            qkv_other(r, (0,))
    with jax.named_scope("a_near_p"):
        for r in (3, 1):
            g1.wait_partner(r)
            qkv_other(r, (1,))
    with jax.named_scope("a_near_own"):
        qkv(3)
        qkv(1)
    with jax.named_scope("a_two"):
        for g in row_groups[2]:
            g1.wait(2, g)
        qkv_other(2, (0,))
    with jax.named_scope("w_ring0"):
        w_near(3, [0])
        w_near(1, [4])
    with jax.named_scope("a_two_p"):
        g1.wait_partner(2)
        qkv_other(2, (1,))
        qkv(2)
    with jax.named_scope("w_ring1"):
        w_near(3, [1])
        w_near(1, [3])
        w_cross()
    with jax.named_scope("a_recv0"):
        receive(0)
    with jax.named_scope("a_early0"):
        top = score(early[0], 0, early)
        top = begin_tile(0, top)
    with jax.named_scope("w_ring2"):
        w_near(3, [2])
        w_near(1, [2])
    with jax.named_scope("a_early1"):
        top = begin_tile(1, top)
        top = begin_tile(2, top)
    with jax.named_scope("w_ring3"):
        w_near(3, [3, 4])
        w_near(1, [0, 1])
    with jax.named_scope("a_early2"):
        top = begin_tile(3, top)
    with jax.named_scope("a_recv3"):
        receive(3)
    with jax.named_scope("w_far0"):
        w_far(0)
        w_far(4)
    with jax.named_scope("a_early3"):
        top = begin_tile(4, top)
    with jax.named_scope("a_recv1"):
        receive(1)
    with jax.named_scope("w_far1"):
        w_far(1)
        w_far(3)
    with jax.named_scope("a_early4"):
        top = begin_tile(5, top)
        begin_tile(6, top, False)
    with jax.named_scope("w_far2"):
        w_far(2)
    with jax.named_scope("a_recv2"):
        receive(2)

    def give(r):
        for p in range(2):
            if r == 0 and p == 0:
                continue
            role = 4 * (r // 4) + (-r % 4) % 4
            pltpu.make_async_remote_copy(
                src_ref=osend.at[2 * r + p],
                dst_ref=att.at[2 * role + p],
                send_sem=asem.at[0],
                recv_sem=asem.at[1],
                device_id={"sp": dev(r % 4, r // 4, p)},
                device_id_type=MESH,
            ).start()

    order = (6, 7, 5, 2, 4, 3, 1, 0)
    def keys(r):
        return late if r in ahead else early + late

    top = score(order[0], 0, keys(order[0]))
    for i, r in enumerate(order):
        if i + 1 < ROLES:
            later = score(order[i + 1], (i + 1) % 2, keys(order[i + 1]))
        end_tile(r, i % 2, top)
        top = later
        if i > 0:
            give(order[i - 1])
        if i == 4:
            with jax.named_scope("w_last0"):
                gw.wait(7, two[0])
                gw.wait(5, two[0])
    with jax.named_scope("t_give"):
        give(order[-1])
        att[0] = osend[0]
    with jax.named_scope("w_last"):
        gw.wait(6, two[1])
        gw.wait(5, two[1])
        gw.wait(7, two[1])
        gw.wait(6, two[0])
    with jax.named_scope("w_partner"):
        pltpu.make_async_remote_copy(
            src_ref=wg.at[:, 1], dst_ref=wg.at[:, 1], send_sem=ssend.at[2], recv_sem=wprecv.at[0],
            device_id={"img": img, "sp": dev(0, 0, 1)}, device_id_type=MESH,
        ).wait_recv()
    with jax.named_scope("t_back"):
        pltpu.make_async_remote_copy(
            src_ref=osend.at[pl.ds(1, 15)], dst_ref=att.at[pl.ds(1, 15)], send_sem=asem.at[0], recv_sem=asem.at[1],
            device_id={"sp": dev(0, 0, 1)}, device_id_type=MESH,
        ).wait_recv()

    for load in loads[8:11]:
        load.wait()
    got = att[...].reshape(D, 128).T
    out = jnp.dot(got, wg[...].reshape(D, D), preferred_element_type=jnp.float32)
    vit = (x_ref[...].astype(jnp.float32) + out + pb_ref[...].reshape(1, D)).astype(jnp.bfloat16)
    vit_ref[...] = vit
    zn = norm_rows(vit.astype(jnp.float32), g2_ref[...].reshape(1, D), b2_ref[...].reshape(1, D))
    for b in range(D // 128):
        zf[b] = zn[:, b * 128 : (b + 1) * 128]
    for j in range(4):
        for b in range(D // 128):
            blk[0, 0, pl.ds(j * 32, 32), pl.ds(b * 128, 128)] = zf[
                b, pl.ds(j, 32, stride=4), :
            ].astype(jnp.bfloat16)

    g2.begin()
    loads[11].wait()

    def fc1(dy, j):
        parts = []
        for ax in range(4):
            r = 4 * dy + (ax + 4 - mx) % 4
            for c in range(2):
                parts.append(blk[r, (c + core) % 2, pl.ds(j * 32, 32)])
        return lax.dot_general(
            fcv[:, j * D : (j + 1) * D],
            jnp.concatenate(parts, axis=0),
            (((1,), (1,)), ((), ())),
            preferred_element_type=jnp.float32,
        )

    def finish(dy, total):
        v = total + jnp.concatenate([fcol[...], fcol[...]], axis=1)
        at = pl.multiple_of(((my + dy) % 2) * 256, 256)
        hid_ref[:, pl.ds(at, 256)] = (0.5 * v * (1.0 + lax.erf(v * (2.0**-0.5)))).astype(jnp.bfloat16)

    with jax.named_scope("b_ring"):
        g2.ring_all()
    with jax.named_scope("b_cross"):
        g2.cross(halves[0])
    with jax.named_scope("b_far0"):
        for i in flow[:4]:
            g2.far(i)
    with jax.named_scope("b_cross1"):
        g2.cross(halves[1])
    with jax.named_scope("b_far1"):
        for i in flow[4:]:
            g2.far(i)
    with jax.named_scope("b_rest"):
        g2.rest()
    def partner(j):
        with jax.named_scope(f"b_partner{j}"):
            for r in (5, 7, 6):
                g2.wait_partner(r, j)

    with jax.named_scope("b_last0"):
        g2.last(pairs[0])
    with jax.named_scope("b_far_p"):
        for r in (0, 3, 1, 2, 4):
            g2.wait_partner(r)
    with jax.named_scope("b_fc1_a"):
        acc[...] = fc1(0, 0) + fc1(0, 1)
    with jax.named_scope("b_last1"):
        g2.last(pairs[1])
    with jax.named_scope("b_fc1_b"):
        finish(0, acc[...] + fc1(0, 2) + fc1(0, 3))
    with jax.named_scope("b_last2"):
        g2.last(pairs[2])
    partner(0)
    with jax.named_scope("b_fc1_c"):
        acc[...] = fc1(1, 0)
    with jax.named_scope("b_last3"):
        g2.last(pairs[3])
    partner(1)
    with jax.named_scope("b_fc1_d"):
        acc[...] += fc1(1, 1)
    partner(2)
    with jax.named_scope("b_fc1_e"):
        acc[...] += fc1(1, 2)
    partner(3)
    with jax.named_scope("b_fc1_f"):
        finish(1, acc[...] + fc1(1, 3))

    with jax.named_scope("drain"):
        for g in (g1, gw, g2):
            g.drain()
        head_weights(0, 3 * HDIM, 0).wait_send()
        pltpu.make_async_remote_copy(
            src_ref=stage, dst_ref=stage, send_sem=hsend.at[1], recv_sem=hrecv.at[2],
            device_id={"img": img, "sp": dev(0, 1, 0)}, device_id_type=MESH,
        ).wait_send()
        pltpu.make_async_remote_copy(
            src_ref=osend.at[pl.ds(1, 15)], dst_ref=att.at[pl.ds(1, 15)], send_sem=asem.at[0], recv_sem=asem.at[1],
            device_id={"sp": dev(0, 0, 1)}, device_id_type=MESH,
        ).wait_send()


def put(vit_ref, hid_ref, vit_hbm, hid_hbm, sem):
    copies = [
        pltpu.make_async_copy(vit_ref, vit_hbm, sem.at[0]),
        pltpu.make_async_copy(hid_ref, hid_hbm, sem.at[1]),
    ]
    for copy in copies:
        copy.start()
    for copy in copies:
        copy.wait()


def per_device(
    patches, pos_ids, norm_gain, norm_bias, qkv_weight, qkv_bias, proj_weight, proj_bias, merge_gain, merge_bias,
    fc1_weight, fc1_bias,
):
    vmem = pl.BlockSpec(memory_space=pltpu.VMEM)
    hbm = pl.BlockSpec(memory_space=pl.ANY)
    bf, f32 = jnp.bfloat16, jnp.float32
    dma = pltpu.SemaphoreType.DMA
    vit, hid = pl.pallas_call(
        kernel,
        out_shape=(pltpu.VMEM((128, D), bf), pltpu.VMEM((SHARE, 512), bf)),
        in_specs=[hbm] * 12,
        out_specs=(vmem, vmem),
        scratch_shapes=[
            pltpu.VMEM((128, D), bf),
            pltpu.VMEM((2, PATCHES), jnp.int32),
            pltpu.VMEM((D,), f32),
            pltpu.VMEM((D,), f32),
            pltpu.VMEM((3, D), f32),
            pltpu.VMEM((D,), f32),
            pltpu.VMEM((D,), f32),
            pltpu.VMEM((D,), f32),
            pltpu.VMEM((SHARE,), f32),
            pltpu.VMEM((4, 2, 128, D), bf),
            pltpu.VMEM((ROLES, 2, 128, D), bf),
            pltpu.VMEM((ROLES, 2, HDIM, D), bf),
            pltpu.VMEM((2 * ROLES, HDIM, 128), bf),
            pltpu.VMEM((2 * ROLES, HDIM, 128), bf),
            pltpu.VMEM((ROLES, 128, 256), bf),
            pltpu.VMEM((ROLES, 256, 128), bf),
            pltpu.VMEM((ROLES, HDIM, 256), bf),
            pltpu.VMEM((2, ROLES, 256, 256), f32),
            pltpu.VMEM((SHARE, HIDDEN), bf),
            pltpu.VMEM((3 * HDIM, D), bf),
            pltpu.VMEM((6, HDIM, 128), f32),
            pltpu.VMEM((SHARE, 128), f32),
            pltpu.VMEM((D // 128, 128, 128), f32),
            pltpu.VMEM((SHARE, 256), f32),
            pltpu.VMEM((7, HDIM, 256), f32),
            pltpu.VMEM((7, 8, 256), f32),
            pltpu.VMEM((3 * HDIM, D), bf),
            pltpu.VMEM((4, 2, 40, 256), f32),
            pltpu.VMEM((4, 3, HDIM, 256), bf),
            pltpu.VMEM((4, HDIM, 256), bf),
            dma((3,)),
            dma((35,)),
            dma((ROLES + 9,)),
            dma((20,)),
            dma((1,)),
            dma((2,)),
            dma((6,)),
            dma((2,)),
            dma((12,)),
        ],
        compiler_params=pltpu.CompilerParams(
            collective_id=0, has_side_effects=True, vmem_limit_bytes=58 * 1024 * 1024
        ),
    )(
        patches,
        pos_ids,
        norm_gain,
        norm_bias,
        qkv_weight.transpose(1, 2, 0).reshape(3 * HDIM, D),
        qkv_bias,
        proj_weight,
        proj_bias,
        merge_gain,
        merge_bias,
        fc1_weight.T,
        fc1_bias,
    )
    vit, hid = pl.pallas_call(
        put,
        out_shape=(jax.ShapeDtypeStruct((128, D), bf), jax.ShapeDtypeStruct((SHARE, 512), bf)),
        in_specs=[vmem, vmem],
        out_specs=(hbm, hbm),
        scratch_shapes=[dma((2,))],
    )(pltpu.with_memory_space_constraint(vit, pltpu.VMEM), pltpu.with_memory_space_constraint(hid, pltpu.VMEM))
    return vit, hid.T


def solution(mesh):
    return jax.shard_map(
        per_device,
        mesh=mesh,
        in_specs=(
            P(("img", "sp"), None),
            P(None, "img"),
            P(),
            P(),
            P(None, None, "sp"),
            P(),
            P("sp", None),
            P(),
            P(),
            P(),
            P(None, "sp"),
            P("sp"),
        ),
        out_specs=(P(("img", "sp"), None), P("img", "sp")),
        check_vma=False,
    )
```

```python
import math

import jax
import jax.numpy as jnp
from jax import lax
from jax.experimental import pallas as pl
from jax.experimental.pallas import tpu as pltpu
from jax.sharding import PartitionSpec as P

MESH = pl.DeviceIdType.MESH
HEADS = 16
D = 1280
HDIM = 80
PATCHES = 2048
HIDDEN = 5120
SHARE = 320
ROLES = 8
SCALE = math.log2(math.e) / math.sqrt(HDIM)


def norm_rows(v, gain, bias):
    mean = jnp.mean(v, axis=-1, keepdims=True)
    cen = v - mean
    var = jnp.mean(cen * cen, axis=-1, keepdims=True)
    return cen * lax.rsqrt(var + 1e-06) * gain + bias


def kernel(
    x_hbm, pos_hbm, g1_hbm, b1_hbm, wq_hbm, bq_hbm, wp_hbm, pb_hbm, g2_hbm, b2_hbm, fc_hbm, fb_hbm,
    vit_ref, hid_ref, x_ref, pos_ref, g1_ref, b1_ref, bq_ref, pb_ref, g2_ref, b2_ref, fb_ref,
    gat, blk, wg, att, osend, qt, kk, vt, sc, fcv, wqv, bcol, fcol, zf, acc, osum, stat,
    wqo, trig, stage, kin, ssend, srecv, precv, wsrecv, wprecv, hsend, hrecv, asem, local,
):
    me = lax.axis_index("sp")
    img, images = lax.axis_index("img"), lax.axis_size("img")
    core = me % 2
    mx = (me // 2) % 4
    my = me // 8

    def dev(dx, dy, p):
        return ((my + dy) % 2) * 8 + ((mx + dx) % 4) * 2 + (core + p) % 2

    barrier = pltpu.get_barrier_semaphore()
    for near in (dev(1, 0, 0), dev(-1, 0, 0), dev(0, 1, 0), dev(0, 0, 1)):
        pl.semaphore_signal(barrier, inc=1, device_id={"img": img, "sp": near}, device_id_type=MESH)
    pl.semaphore_signal(barrier, inc=1, device_id={"img": (img + images // 2) % images, "sp": dev(0, 1, 0)}, device_id_type=MESH)

    loads = [
        (x_hbm, x_ref), (g1_hbm, g1_ref), (b1_hbm, b1_ref), (wq_hbm, wqv), (wp_hbm, wg.at[0, 0]), (bq_hbm, bq_ref),
        (fb_hbm, fb_ref), (pos_hbm, pos_ref), (pb_hbm, pb_ref), (g2_hbm, g2_ref), (b2_hbm, b2_ref), (fc_hbm, fcv),
    ]
    loads = [pltpu.make_async_copy(src, dst, local.at[i]) for i, (src, dst) in enumerate(loads)]
    for load in loads:
        load.start()
    with jax.named_scope("s_load"):
        for load in loads[:3]:
            load.wait()

    ln_scope = jax.named_scope("s_ln")
    ln_scope.__enter__()
    xf = x_ref[...].astype(jnp.float32)
    normed = norm_rows(xf, g1_ref[...].reshape(1, D), b1_ref[...].reshape(1, D)).astype(jnp.bfloat16)
    gat[0, 0] = normed
    ln_scope.__exit__(None, None, None)

    with jax.named_scope("s_bar"):
        pl.semaphore_wait(barrier, 5)

    class Gather:
        def __init__(self, ref, up, down, across, flow, groups, parts, srecv, precv, ssend):
            self.ref, self.up, self.down, self.across, self.flow = ref, up, down, across, flow
            self.groups, self.parts, self.srecv, self.precv, self.ssend = groups, parts, srecv, precv, ssend
            self.rows, self.here, self.sem = 0, {}, {}
            for r in sorted(groups):
                for g in groups[r]:
                    for i in g:
                        self.sem[r, i] = len(set(self.sem.values())) if i == g[0] else self.sem[r, g[0]]

        def copy(self, src, dst, size, at, rsem, dx, dy, p, other=False):
            return pltpu.make_async_remote_copy(
                src_ref=self.ref.at[src[0], src[1], pl.ds(at, size)],
                dst_ref=self.ref.at[dst[0], dst[1], pl.ds(at, size)],
                send_sem=self.ssend,
                recv_sem=rsem,
                device_id={"img": (img + images // 2) % images if other else img, "sp": dev(dx, dy, p)},
                device_id_type=MESH,
            )

        def pass_on(self, r, i, dx, dy, other=False):
            role = 4 * ((r // 4 + dy) % 2) + (r % 4 - dx) % 4
            self.copy((r, 0), (role, 0), 16, 16 * i, self.srecv.at[self.sem[role, i]], dx, dy, 0, other).start()
            self.rows += 16

        def which(self, r, which):
            return which if r in (5, 6, 7) else 0

        def slot(self, r, which):
            return 0 if self.precv is wprecv else (3 * (r - 5) + which - 1 + ROLES if which else r)

        def share(self, r, part):
            at, size, which = self.parts[part]
            which = self.which(r, which)
            self.copy((r, 0), (r, 1), size, at, self.precv.at[self.slot(r, which)], 0, 0, 1).start()
            self.rows += size

        def wait(self, r, g):
            self.copy((r, 0), (r, 0), 16 * len(g), 16 * g[0], self.srecv.at[self.sem[r, g[0]]], 0, 0, 1).wait_recv()
            assert list(g) in [list(v) for v in self.groups[r]]
            if r in (1, 3) and self.across in g:
                self.pass_on(r, self.across, 0, 1)
            here = self.here.setdefault(r, set())
            for part, (at, size, _) in enumerate(self.parts):
                mine = set(range(at // 16, (at + size) // 16))
                if mine <= here | set(g) and not mine <= here:
                    self.share(r, part)
            here.update(g)

        def wait_partner(self, r, which=0):
            size = sum(v[1] for v in self.parts if self.which(r, v[2]) == which)
            at = min(v[0] for v in self.parts if self.which(r, v[2]) == which)
            self.copy((r, 1), (r, 1), size, at, self.precv.at[self.slot(r, which)], 0, 0, 1).wait_recv()

        def own(self, lo, hi):
            for a, b in list(zip(self.up + self.down, self.down + self.up))[lo:hi]:
                self.pass_on(0, a, 1, 0)
                self.pass_on(0, b, -1, 0)

        def share_own(self):
            for part in range(len(self.parts)):
                self.share(0, part)

        def begin(self):
            self.own(0, 2)
            for n, c in enumerate(self.flow):
                self.pass_on(0, c, 0, 1)
                if n in (1, 3, 5, 7):
                    self.own(2 + n // 2, 3 + n // 2)
            self.share_own()

        def ring_all(self):
            for n, (i, j) in enumerate(zip(self.up, self.down)):
                self.ring(3, i)
                self.ring(1, j)
                if n in (1, 3):
                    self.own(6 + n // 2, 7 + n // 2)

        def ring(self, r, *g):
            self.wait(r, list(g))
            for i in g:
                self.pass_on(r, i, 1 if r == 3 else -1, 0)

        def cross(self, g):
            self.wait(4, g)
            for i in g:
                if i != self.across:
                    self.pass_on(4, i, 1, 0)
                    self.pass_on(4, i, -1, 0)

        def rest(self):
            for r, done in ((3, self.up), (1, self.down)):
                for g in self.groups[r]:
                    if g[0] not in done:
                        self.wait(r, g)

        def far(self, i):
            self.wait(2, [i])
            self.pass_on(2, i, 0, 1)

        def last(self, g):
            for r in (5, 7, 6):
                self.wait(r, g)

        def drain(self):
            total = self.ref.shape[0] * self.ref.shape[1] * self.ref.shape[2]
            assert self.rows <= total
            flat = self.ref.reshape(total, D).at[pl.ds(0, self.rows)]
            pltpu.make_async_remote_copy(
                src_ref=flat, dst_ref=flat, send_sem=self.ssend, recv_sem=self.precv.at[0],
                device_id={"sp": dev(0, 0, 1)}, device_id_type=MESH,
            ).wait_send()

    halves = [[0, 1, 2, 3], [4, 5, 6, 7]]
    pairs = [[0, 1], [2, 3], [4, 5], [6, 7]]
    groups = {
        1: [[2], [3], [6], [7], [0, 1], [4, 5]],
        2: [[i] for i in range(8)],
        3: [[0], [1], [4], [5], [2, 3], [6], [7]],
        4: halves, 5: pairs, 6: pairs, 7: pairs,
    }
    flow = [0, 2, 1, 3, 4, 6, 5, 7]
    big = ([0, 1, 4, 5], [2, 3, 6, 7], 7, flow, groups)
    row_groups = {
        1: [[2, 3], [6, 7], [0, 1], [4, 5]],
        2: [[0, 1], [2, 3], [4, 5], [6, 7]],
        3: [[0, 1], [4, 5], [2, 3], [6, 7]],
    }
    g1 = Gather(
        gat, [0, 1, 4, 5], [2, 3, 6, 7], None, None, row_groups, [(32 * j, 32, 0) for j in range(4)], srecv, precv,
        ssend.at[0],
    )
    g2 = Gather(blk, *big, [(32 * j, 32, j) for j in range(4)], srecv, precv, ssend.at[1])
    whole = [[0, 1, 2, 3, 4]]
    two = [[0, 1, 2], [3, 4]]
    wgroups = {
        1: [[4], [3], [2], [0, 1]],
        2: [[i] for i in range(5)],
        3: [[0], [1], [2], [3, 4]],
        4: whole, 5: two, 6: two, 7: two,
    }
    gw = Gather(wg, [0, 1, 2], [4, 3], None, None, wgroups, [(0, 48, 0), (48, 32, 0)], wsrecv, wprecv, ssend.at[2])

    def w_near(r, g):
        gw.wait(r, g)
        for i in g:
            if i in (gw.up if r == 3 else gw.down):
                gw.pass_on(r, i, 1 if r == 3 else -1, 0)
        for i in g:
            if r == 3 and i != 4:
                gw.pass_on(r, i, 0, 1, True)

    def w_cross():
        gw.wait(4, whole[0])
        gw.pass_on(4, 4, 1, 0)
        for i in range(5):
            gw.pass_on(4, i, -1, 0)

    def w_far(i):
        gw.wait(2, [i])
        gw.pass_on(2, i, 0, 1, True)

    def head_weights(at, size, sem, other=False):
        return pltpu.make_async_remote_copy(
            src_ref=wqv.at[pl.ds(at, size)], dst_ref=wqo.at[pl.ds(at, size)], send_sem=hsend.at[0], recv_sem=hrecv.at[sem],
            device_id={"img": (img + images // 2) % images if other else img, "sp": dev(0, 1, 0)}, device_id_type=MESH,
        )

    g1.own(0, 8)
    loads[3].wait()
    for i in range(15):
        head_weights(16 * i, 16, 0 if i < 10 else 1, i % 2 == 0).start()
    loads[4].wait()
    for i in range(5):
        gw.pass_on(0, i, 0, 1, True)
    g1.share_own()
    gw.share_own()

    for load in loads[5:8]:
        load.wait()
    lane = lax.broadcasted_iota(jnp.int32, (HDIM, D), 1)
    sub = lax.broadcasted_iota(jnp.int32, (HDIM, D), 0)
    for n, head in enumerate((me, dev(0, 1, 0))):
        mine = lane == sub + head * HDIM
        for c in range(3):
            col = jnp.sum(jnp.where(mine, bq_ref[c : c + 1, :], 0.0), axis=1, keepdims=True)
            bcol[3 * n + c] = jnp.broadcast_to(col, (HDIM, 128))
    same = lax.broadcasted_iota(jnp.int32, (SHARE, SHARE), 0) == lax.broadcasted_iota(
        jnp.int32, (SHARE, SHARE), 1
    )
    col = jnp.sum(jnp.where(same, fb_ref[...].reshape(1, SHARE), 0.0), axis=1, keepdims=True)
    fcol[...] = jnp.broadcast_to(col, (SHARE, 128))
    for r in range(4):
        at = [pl.multiple_of(dev(r, 0, p) * 128, 128) for p in range(2)]
        prow = jnp.concatenate([pos_ref[0:1, pl.ds(a, 128)] for a in at], axis=1).astype(jnp.float32)
        pcol = jnp.concatenate([pos_ref[1:2, pl.ds(a, 128)] for a in at], axis=1).astype(jnp.float32)
        row = lax.broadcasted_iota(jnp.int32, (40, 256), 0)
        power = jnp.where(row < 20, row, row - 20).astype(jnp.float32)
        inv = jnp.exp2(power * (-math.log2(10000.0) / 20.0))
        angle = jnp.where(row < 20, prow, pcol) * inv
        trig[r, 0] = jnp.cos(angle)
        trig[r, 1] = jnp.sin(angle)
    for r in range(4, ROLES):
        qt[r, HDIM:128] = jnp.zeros((128 - HDIM, 256), jnp.bfloat16)

    def project(weights, r, ps):
        rows = gat[r, ps[0] : ps[-1] + 1].reshape(128 * len(ps), D)
        return lax.dot_general(weights, rows, (((1,), (1,)), ((), ())), preferred_element_type=jnp.float32)

    def finish_head(v, r, ps, n, c):
        v = v + jnp.concatenate([bcol[3 * n + c]] * len(ps), axis=1)
        if c == 2:
            return v
        cos, sin = (trig[r, t, :, pl.ds(128 * ps[0], 128 * len(ps))] for t in range(2))
        lo, hi = v[:40], v[40:]
        return jnp.concatenate([lo * cos - hi * sin, hi * cos + lo * sin], axis=0)

    def turned_keys(k):
        return jnp.concatenate([k, jnp.zeros((128 - HDIM, 256), jnp.float32)], axis=0).T.astype(jnp.bfloat16)

    def qkv(r):
        out = project(wqv[...], r, (0, 1))
        q, k, v = (finish_head(out[80 * c : 80 * c + 80], r, (0, 1), 0, c) for c in range(3))
        qt[r] = jnp.concatenate([q, jnp.zeros((128 - HDIM, 256), jnp.float32)], axis=0).astype(jnp.bfloat16)
        kk[r] = turned_keys(k)
        vt[r] = v.astype(jnp.bfloat16)

    def qkv_other(r, ps, cs=(0, 1, 2)):
        out = project(wqo[80 * cs[0] : 80 * cs[-1] + 80], r, ps)
        lanes = pl.ds(128 * ps[0], 128 * len(ps))
        for n, c in enumerate(cs):
            stage[r, c, :, lanes] = finish_head(out[80 * n : 80 * n + 80], r, ps, 1, c).astype(jnp.bfloat16)
        for c in cs:
            dst = (qt.at[4 + r, pl.ds(0, HDIM), lanes], kin.at[r, :, lanes], vt.at[4 + r, :, lanes])[c]
            pltpu.make_async_remote_copy(
                src_ref=stage.at[r, c, :, lanes], dst_ref=dst, send_sem=hsend.at[1], recv_sem=hrecv.at[2 + r],
                device_id={"img": img, "sp": dev(0, 1, 0)}, device_id_type=MESH,
            ).start()

    def receive(r):
        pltpu.make_async_remote_copy(
            src_ref=stage.at[r], dst_ref=stage.at[r], send_sem=hsend.at[1], recv_sem=hrecv.at[2 + r],
            device_id={"img": img, "sp": dev(0, 1, 0)}, device_id_type=MESH,
        ).wait_recv()
        kk[4 + r] = turned_keys(kin[r].astype(jnp.float32))

    early, late, ahead = (0, 3, 1, 2, 4), (7, 5, 6), (0, 3, 1, 2, 4, 7, 5)

    def score(r, slot, keys):
        top = None
        for n, c in enumerate(keys):
            s = jnp.dot(kk[c], qt[r], preferred_element_type=jnp.float32)
            sc[slot, n] = s
            m = jnp.max(s.reshape(32, 8, 256), axis=0)
            top = m if top is None else jnp.maximum(top, m)
        return jnp.max(top, axis=0, keepdims=True) * SCALE

    def weigh(slot, keys, top):
        total, out = None, None
        for n, c in enumerate(keys):
            w = jnp.exp2(sc[slot, n] * SCALE - top)
            s = jnp.sum(w.reshape(32, 8, 256), axis=0)
            o = jnp.dot(vt[c], w.astype(jnp.bfloat16), preferred_element_type=jnp.float32)
            total = s if total is None else total + s
            out = o if out is None else out + o
        return jnp.sum(total, axis=0, keepdims=True), out

    def begin_tile(n, top, more=True):
        later = score(ahead[n + 1], (n + 1) % 2, early) if more else None
        total, out = weigh(n % 2, early, top)
        osum[n] = out
        stat[n, 0:1] = top
        stat[n, 1:2] = total
        return later

    def end_tile(r, slot, top):
        if r in ahead:
            n = ahead.index(r)
            before = stat[n, 0:1]
            both = jnp.maximum(before, top)
            total, out = weigh(slot, late, both)
            old = jnp.exp2(before - both)
            total, out = total + stat[n, 1:2] * old, out + osum[n] * old
        else:
            total, out = weigh(slot, early + late, top)
        out = (out / total).astype(jnp.bfloat16)
        for p in range(2):
            osend[2 * r + p] = out[:, p * 128 : (p + 1) * 128]

    with jax.named_scope("a_own"):
        g1.wait_partner(0)
        qkv(0)
    with jax.named_scope("a_ring"):
        g1.ring(3, 0, 1)
        g1.ring(1, 2, 3)
        g1.ring(3, 4, 5)
        g1.ring(1, 6, 7)
        gw.own(0, 5)
    with jax.named_scope("a_other0"):
        head_weights(0, 160, 0).wait_recv()
        qkv_other(0, (0, 1), (0, 1))
    with jax.named_scope("a_rest"):
        for r in (3, 1):
            g1.wait(r, row_groups[r][2])
            g1.wait(r, row_groups[r][3])
    with jax.named_scope("a_other0v"):
        head_weights(160, 80, 1).wait_recv()
        qkv_other(0, (0, 1), (2,))
    with jax.named_scope("a_near"):
        for r in (3, 1):
            qkv_other(r, (0,))
    with jax.named_scope("a_near_p"):
        for r in (3, 1):
            g1.wait_partner(r)
            qkv_other(r, (1,))
    with jax.named_scope("a_near_own"):
        qkv(3)
        qkv(1)
    with jax.named_scope("a_two"):
        for g in row_groups[2]:
            g1.wait(2, g)
        qkv_other(2, (0,))
    with jax.named_scope("w_ring0"):
        w_near(3, [0])
        w_near(1, [4])
    with jax.named_scope("a_two_p"):
        g1.wait_partner(2)
        qkv_other(2, (1,))
        qkv(2)
    with jax.named_scope("w_ring1"):
        w_near(3, [1])
        w_near(1, [3])
        w_cross()
    with jax.named_scope("a_recv0"):
        receive(0)
    with jax.named_scope("a_early0"):
        top = score(early[0], 0, early)
        top = begin_tile(0, top)
    with jax.named_scope("w_ring2"):
        w_near(3, [2])
        w_near(1, [2])
    with jax.named_scope("a_early1"):
        top = begin_tile(1, top)
        top = begin_tile(2, top)
    with jax.named_scope("w_ring3"):
        w_near(3, [3, 4])
        w_near(1, [0, 1])
    with jax.named_scope("a_early2"):
        top = begin_tile(3, top)
    with jax.named_scope("a_recv3"):
        receive(3)
    with jax.named_scope("w_far0"):
        w_far(0)
        w_far(4)
    with jax.named_scope("a_early3"):
        top = begin_tile(4, top)
    with jax.named_scope("a_recv1"):
        receive(1)
    with jax.named_scope("w_far1"):
        w_far(1)
        w_far(3)
    with jax.named_scope("a_early4"):
        top = begin_tile(5, top)
        begin_tile(6, top, False)
    with jax.named_scope("w_far2"):
        w_far(2)
    with jax.named_scope("a_recv2"):
        receive(2)

    def give(r):
        for p in range(2):
            if r == 0 and p == 0:
                continue
            role = 4 * (r // 4) + (-r % 4) % 4
            pltpu.make_async_remote_copy(
                src_ref=osend.at[2 * r + p],
                dst_ref=att.at[2 * role + p],
                send_sem=asem.at[0],
                recv_sem=asem.at[1],
                device_id={"sp": dev(r % 4, r // 4, p)},
                device_id_type=MESH,
            ).start()

    order = (2, 7, 6, 5, 4, 3, 1, 0)
    def keys(r):
        return late if r in ahead else early + late

    top = score(order[0], 0, keys(order[0]))
    for i, r in enumerate(order):
        if i + 1 < ROLES:
            later = score(order[i + 1], (i + 1) % 2, keys(order[i + 1]))
        end_tile(r, i % 2, top)
        top = later
        if i > 0:
            give(order[i - 1])
        if i == 4:
            with jax.named_scope("w_last0"):
                gw.wait(7, two[0])
                gw.wait(5, two[0])
    with jax.named_scope("t_give"):
        give(order[-1])
        att[0] = osend[0]
    with jax.named_scope("w_last"):
        gw.wait(6, two[1])
        gw.wait(5, two[1])
        gw.wait(7, two[1])
        gw.wait(6, two[0])
    with jax.named_scope("w_partner"):
        pltpu.make_async_remote_copy(
            src_ref=wg.at[:, 1], dst_ref=wg.at[:, 1], send_sem=ssend.at[2], recv_sem=wprecv.at[0],
            device_id={"img": img, "sp": dev(0, 0, 1)}, device_id_type=MESH,
        ).wait_recv()
    with jax.named_scope("t_back"):
        pltpu.make_async_remote_copy(
            src_ref=osend.at[pl.ds(1, 15)], dst_ref=att.at[pl.ds(1, 15)], send_sem=asem.at[0], recv_sem=asem.at[1],
            device_id={"sp": dev(0, 0, 1)}, device_id_type=MESH,
        ).wait_recv()

    for load in loads[8:11]:
        load.wait()
    got = att[...].reshape(D, 128).T
    out = jnp.dot(got, wg[...].reshape(D, D), preferred_element_type=jnp.float32)
    vit = (x_ref[...].astype(jnp.float32) + out + pb_ref[...].reshape(1, D)).astype(jnp.bfloat16)
    vit_ref[...] = vit
    zn = norm_rows(vit.astype(jnp.float32), g2_ref[...].reshape(1, D), b2_ref[...].reshape(1, D))
    for b in range(D // 128):
        zf[b] = zn[:, b * 128 : (b + 1) * 128]
    for j in range(4):
        for b in range(D // 128):
            blk[0, 0, pl.ds(j * 32, 32), pl.ds(b * 128, 128)] = zf[
                b, pl.ds(j, 32, stride=4), :
            ].astype(jnp.bfloat16)

    g2.begin()
    loads[11].wait()

    def fc1(dy, j):
        parts = []
        for ax in range(4):
            r = 4 * dy + (ax + 4 - mx) % 4
            for c in range(2):
                parts.append(blk[r, (c + core) % 2, pl.ds(j * 32, 32)])
        return lax.dot_general(
            fcv[:, j * D : (j + 1) * D],
            jnp.concatenate(parts, axis=0),
            (((1,), (1,)), ((), ())),
            preferred_element_type=jnp.float32,
        )

    def finish(dy, total):
        v = total + jnp.concatenate([fcol[...], fcol[...]], axis=1)
        at = pl.multiple_of(((my + dy) % 2) * 256, 256)
        hid_ref[:, pl.ds(at, 256)] = (0.5 * v * (1.0 + lax.erf(v * (2.0**-0.5)))).astype(jnp.bfloat16)

    with jax.named_scope("b_ring"):
        g2.ring_all()
    with jax.named_scope("b_cross"):
        g2.cross(halves[0])
    with jax.named_scope("b_far0"):
        for i in flow[:4]:
            g2.far(i)
    with jax.named_scope("b_cross1"):
        g2.cross(halves[1])
    with jax.named_scope("b_far1"):
        for i in flow[4:]:
            g2.far(i)
    with jax.named_scope("b_rest"):
        g2.rest()
    def partner(j):
        with jax.named_scope(f"b_partner{j}"):
            for r in (5, 7, 6):
                g2.wait_partner(r, j)

    with jax.named_scope("b_last0"):
        g2.last(pairs[0])
    with jax.named_scope("b_far_p"):
        for r in (0, 3, 1, 2, 4):
            g2.wait_partner(r)
    with jax.named_scope("b_fc1_a"):
        acc[...] = fc1(0, 0) + fc1(0, 1)
    with jax.named_scope("b_last1"):
        g2.last(pairs[1])
    with jax.named_scope("b_fc1_b"):
        finish(0, acc[...] + fc1(0, 2) + fc1(0, 3))
    with jax.named_scope("b_last2"):
        g2.last(pairs[2])
    partner(0)
    with jax.named_scope("b_fc1_c"):
        acc[...] = fc1(1, 0)
    with jax.named_scope("b_last3"):
        g2.last(pairs[3])
    partner(1)
    with jax.named_scope("b_fc1_d"):
        acc[...] += fc1(1, 1)
    partner(2)
    with jax.named_scope("b_fc1_e"):
        acc[...] += fc1(1, 2)
    partner(3)
    with jax.named_scope("b_fc1_f"):
        finish(1, acc[...] + fc1(1, 3))

    with jax.named_scope("drain"):
        for g in (g1, gw, g2):
            g.drain()
        head_weights(0, 3 * HDIM, 0).wait_send()
        pltpu.make_async_remote_copy(
            src_ref=stage, dst_ref=stage, send_sem=hsend.at[1], recv_sem=hrecv.at[2],
            device_id={"img": img, "sp": dev(0, 1, 0)}, device_id_type=MESH,
        ).wait_send()
        pltpu.make_async_remote_copy(
            src_ref=osend.at[pl.ds(1, 15)], dst_ref=att.at[pl.ds(1, 15)], send_sem=asem.at[0], recv_sem=asem.at[1],
            device_id={"sp": dev(0, 0, 1)}, device_id_type=MESH,
        ).wait_send()


def put(vit_ref, hid_ref, vit_hbm, hid_hbm, sem):
    copies = [
        pltpu.make_async_copy(vit_ref, vit_hbm, sem.at[0]),
        pltpu.make_async_copy(hid_ref, hid_hbm, sem.at[1]),
    ]
    for copy in copies:
        copy.start()
    for copy in copies:
        copy.wait()


def per_device(
    patches, pos_ids, norm_gain, norm_bias, qkv_weight, qkv_bias, proj_weight, proj_bias, merge_gain, merge_bias,
    fc1_weight, fc1_bias,
):
    vmem = pl.BlockSpec(memory_space=pltpu.VMEM)
    hbm = pl.BlockSpec(memory_space=pl.ANY)
    bf, f32 = jnp.bfloat16, jnp.float32
    dma = pltpu.SemaphoreType.DMA
    vit, hid = pl.pallas_call(
        kernel,
        out_shape=(pltpu.VMEM((128, D), bf), pltpu.VMEM((SHARE, 512), bf)),
        in_specs=[hbm] * 12,
        out_specs=(vmem, vmem),
        scratch_shapes=[
            pltpu.VMEM((128, D), bf),
            pltpu.VMEM((2, PATCHES), jnp.int32),
            pltpu.VMEM((D,), f32),
            pltpu.VMEM((D,), f32),
            pltpu.VMEM((3, D), f32),
            pltpu.VMEM((D,), f32),
            pltpu.VMEM((D,), f32),
            pltpu.VMEM((D,), f32),
            pltpu.VMEM((SHARE,), f32),
            pltpu.VMEM((4, 2, 128, D), bf),
            pltpu.VMEM((ROLES, 2, 128, D), bf),
            pltpu.VMEM((ROLES, 2, HDIM, D), bf),
            pltpu.VMEM((2 * ROLES, HDIM, 128), bf),
            pltpu.VMEM((2 * ROLES, HDIM, 128), bf),
            pltpu.VMEM((ROLES, 128, 256), bf),
            pltpu.VMEM((ROLES, 256, 128), bf),
            pltpu.VMEM((ROLES, HDIM, 256), bf),
            pltpu.VMEM((2, ROLES, 256, 256), f32),
            pltpu.VMEM((SHARE, HIDDEN), bf),
            pltpu.VMEM((3 * HDIM, D), bf),
            pltpu.VMEM((6, HDIM, 128), f32),
            pltpu.VMEM((SHARE, 128), f32),
            pltpu.VMEM((D // 128, 128, 128), f32),
            pltpu.VMEM((SHARE, 256), f32),
            pltpu.VMEM((7, HDIM, 256), f32),
            pltpu.VMEM((7, 8, 256), f32),
            pltpu.VMEM((3 * HDIM, D), bf),
            pltpu.VMEM((4, 2, 40, 256), f32),
            pltpu.VMEM((4, 3, HDIM, 256), bf),
            pltpu.VMEM((4, HDIM, 256), bf),
            dma((3,)),
            dma((35,)),
            dma((ROLES + 9,)),
            dma((20,)),
            dma((1,)),
            dma((2,)),
            dma((6,)),
            dma((2,)),
            dma((12,)),
        ],
        compiler_params=pltpu.CompilerParams(
            collective_id=0, has_side_effects=True, vmem_limit_bytes=58 * 1024 * 1024
        ),
    )(
        patches,
        pos_ids,
        norm_gain,
        norm_bias,
        qkv_weight.transpose(1, 2, 0).reshape(3 * HDIM, D),
        qkv_bias,
        proj_weight,
        proj_bias,
        merge_gain,
        merge_bias,
        fc1_weight.T,
        fc1_bias,
    )
    vit, hid = pl.pallas_call(
        put,
        out_shape=(jax.ShapeDtypeStruct((128, D), bf), jax.ShapeDtypeStruct((SHARE, 512), bf)),
        in_specs=[vmem, vmem],
        out_specs=(hbm, hbm),
        scratch_shapes=[dma((2,))],
    )(pltpu.with_memory_space_constraint(vit, pltpu.VMEM), pltpu.with_memory_space_constraint(hid, pltpu.VMEM))
    return vit, hid.T


def solution(mesh):
    return jax.shard_map(
        per_device,
        mesh=mesh,
        in_specs=(
            P(("img", "sp"), None),
            P(None, "img"),
            P(),
            P(),
            P(None, None, "sp"),
            P(),
            P("sp", None),
            P(),
            P(),
            P(),
            P(None, "sp"),
            P("sp"),
        ),
        out_specs=(P(("img", "sp"), None), P("img", "sp")),
        check_vma=False,
    )
```
